8 devices in a mesh: dp: 1 (over z), tp: 8 (over y, x, core).
Axes of the slice: x: 2, y: 2, z: 1, core: 2. Of those that a mesh axis runs over, the one named last changes fastest.
Arguments:
- hidden: bfloat16 [32, 1536], P('dp')
- lengths: int32 [32], P('dp')
- choice: int32 [2, 32, 8], P(None, 'dp')
- keys_one: bfloat16 [32, 128, 8, 64], P('dp', 'tp')
- vals_one: bfloat16 [32, 128, 8, 64], P('dp', 'tp')
- keys_two: bfloat16 [32, 128, 8, 64], P('dp', 'tp')
- vals_two: bfloat16 [32, 128, 8, 64], P('dp', 'tp')
- g_attn: bfloat16 [2, 1536], replicated
- w_q: bfloat16 [2, 1536, 1536], P(None, None, 'tp')
- w_k: bfloat16 [2, 1536, 512], P(None, None, 'tp')
- w_v: bfloat16 [2, 1536, 512], P(None, None, 'tp')
- w_o: bfloat16 [2, 1536, 1536], P(None, 'tp')
- g_mlp: bfloat16 [2, 1536], replicated
- w_router: bfloat16 [2, 1536, 40], replicated
- w_gate: bfloat16 [2, 40, 1536, 512], P(None, None, None, 'tp')
- w_up: bfloat16 [2, 40, 1536, 512], P(None, None, None, 'tp')
- w_down: bfloat16 [2, 40, 512, 1536], P(None, None, 'tp')
Outputs:
- output 1: bfloat16 [32, 1536], P('dp')
- output 2: bfloat16 [32, 128, 8, 64], P('dp', None, 'tp')
- output 3: bfloat16 [32, 128, 8, 64], P('dp', None, 'tp')
- output 4: bfloat16 [32, 128, 8, 64], P('dp', None, 'tp')
- output 5: bfloat16 [32, 128, 8, 64], P('dp', None, 'tp')
All inputs are finite; a program needn't handle non-finite values.
Results may differ from the reference program's by a relative error of at most 0.02.
Values are sent between devices in bfloat16 or wider.
A program may use at most 1 GiB of HBM per device.

```python
import jax
import jax.numpy as jnp
from jax import lax

BATCH = 32
SEQ = 128
D = 1536
HEADS = 24
KV_HEADS = 8
HEAD = 64
FF = 512
EXPERTS = 40
TOP = 8
LAYERS = 2
EPS = 1e-5
THETA = 1000000.0


def weight_draw(key, shape, fan_in, gain_mult):
    return (jax.random.normal(key, shape, jnp.float32) * (gain_mult * fan_in ** -0.5)).astype(jnp.bfloat16)


def value_walk(key, cache_shape):
    step_key, noise_key = jax.random.split(key)
    walk_steps = jax.random.normal(step_key, cache_shape, jnp.float32) * SEQ ** -0.5
    noise_part = 0.5 * jax.random.normal(noise_key, cache_shape, jnp.float32)
    return (jnp.cumsum(walk_steps, axis=1) + noise_part).astype(jnp.bfloat16)


def setup_inputs(seed: int = 0, part: int = 0) -> dict:
    base_key = jax.random.key(seed)
    shared = jax.random.split(base_key, 11)
    local_keys = jax.random.split(jax.random.fold_in(base_key, part), 9)
    cache_shape = (BATCH, SEQ, KV_HEADS, HEAD)
    hidden = jax.random.normal(local_keys[0], (BATCH, D), jnp.float32).astype(jnp.bfloat16)
    drawn_lens = jax.random.randint(local_keys[1], (BATCH,), 0, SEQ)
    full_row = jax.random.randint(local_keys[2], (), 0, BATCH)
    lengths = jnp.where(jnp.arange(BATCH) == full_row, SEQ - 1, drawn_lens).astype(jnp.int32)
    rank_score = jax.random.randint(local_keys[3], (LAYERS, BATCH, EXPERTS), 0, 2 ** 20) * EXPERTS + jnp.arange(EXPERTS)
    choice = lax.top_k(rank_score, TOP)[1].astype(jnp.int32)
    return {
        'hidden': hidden,
        'lengths': lengths,
        'choice': choice,
        'keys_one': jax.random.normal(local_keys[4], cache_shape, jnp.float32).astype(jnp.bfloat16),
        'vals_one': value_walk(local_keys[5], cache_shape),
        'keys_two': jax.random.normal(local_keys[6], cache_shape, jnp.float32).astype(jnp.bfloat16),
        'vals_two': value_walk(local_keys[7], cache_shape),
        'g_attn': (1.0 + 0.3 * jax.random.normal(shared[0], (LAYERS, D), jnp.float32)).astype(jnp.bfloat16),
        'w_q': weight_draw(shared[1], (LAYERS, D, HEADS * HEAD), D, 1.0),
        'w_k': weight_draw(shared[2], (LAYERS, D, KV_HEADS * HEAD), D, 1.0),
        'w_v': weight_draw(shared[3], (LAYERS, D, KV_HEADS * HEAD), D, 1.0),
        'w_o': weight_draw(shared[4], (LAYERS, HEADS * HEAD, D), HEADS * HEAD, 1.0),
        'g_mlp': (1.0 + 0.3 * jax.random.normal(shared[5], (LAYERS, D), jnp.float32)).astype(jnp.bfloat16),
        'w_router': weight_draw(shared[6], (LAYERS, D, EXPERTS), D, 2.0),
        'w_gate': weight_draw(shared[7], (LAYERS, EXPERTS, D, FF), D, 1.0),
        'w_up': weight_draw(shared[8], (LAYERS, EXPERTS, D, FF), D, 1.0),
        'w_down': weight_draw(shared[9], (LAYERS, EXPERTS, FF, D), FF, 2.0),
    }


def rms_norm(tensor, gain_vec):
    tensor_f = tensor.astype(jnp.float32)
    scale = lax.rsqrt(jnp.mean(tensor_f * tensor_f, axis=-1, keepdims=True) + EPS)
    return (tensor_f * scale * gain_vec.astype(jnp.float32)).astype(jnp.bfloat16)


def apply_rope(tensor, lengths):
    head_dim = tensor.shape[-1]
    half_dim = head_dim // 2
    inv_freq = THETA ** (-2.0 * jnp.arange(half_dim, dtype=jnp.float32) / head_dim)
    angle = lengths.astype(jnp.float32)[:, None] * inv_freq[None, :]
    cos_part = jnp.cos(angle)[:, None, :]
    sin_part = jnp.sin(angle)[:, None, :]
    lower_half = tensor[..., :half_dim]
    upper_half = tensor[..., half_dim:]
    return jnp.concatenate([lower_half * cos_part - upper_half * sin_part, upper_half * cos_part + lower_half * sin_part], axis=-1)


def decode_layer(hidden, lengths, choice, key_cache, val_cache, g_attn, w_q, w_k, w_v, w_o, g_mlp, w_router, w_gate, w_up, w_down):
    batch_rows = hidden.shape[0]
    seq_len = key_cache.shape[1]
    normed = rms_norm(hidden, g_attn)
    query_rot = apply_rope(jnp.dot(normed, w_q, preferred_element_type=jnp.float32).reshape(batch_rows, HEADS, HEAD), lengths).astype(jnp.bfloat16)
    key_new = apply_rope(jnp.dot(normed, w_k, preferred_element_type=jnp.float32).reshape(batch_rows, KV_HEADS, HEAD), lengths).astype(jnp.bfloat16)
    val_new = jnp.dot(normed, w_v, preferred_element_type=jnp.float32).astype(jnp.bfloat16).reshape(batch_rows, KV_HEADS, HEAD)
    positions = jnp.arange(seq_len)
    is_new = (positions[None, :] == lengths[:, None])[:, :, None, None]
    key_cache = jnp.where(is_new, key_new[:, None], key_cache)
    val_cache = jnp.where(is_new, val_new[:, None], val_cache)
    query_grp = query_rot.reshape(batch_rows, KV_HEADS, HEADS // KV_HEADS, HEAD)
    scores = jnp.einsum('bgrd,bsgd->bgrs', query_grp.astype(jnp.float32), key_cache.astype(jnp.float32)) * HEAD ** -0.5
    is_valid = (positions[None, :] <= lengths[:, None])[:, None, None, :]
    attn_prob = jax.nn.softmax(jnp.where(is_valid, scores, -1e30), axis=-1).astype(jnp.bfloat16)
    attn_vec = jnp.einsum('bgrs,bsgd->bgrd', attn_prob.astype(jnp.float32), val_cache.astype(jnp.float32)).astype(jnp.bfloat16).reshape(batch_rows, HEADS * HEAD)
    x_mid = (hidden.astype(jnp.float32) + jnp.dot(attn_vec, w_o, preferred_element_type=jnp.float32)).astype(jnp.bfloat16)
    normed_mid = rms_norm(x_mid, g_mlp)
    logits = jnp.dot(normed_mid, w_router, preferred_element_type=jnp.float32)
    onehot = (choice[:, :, None] == jnp.arange(EXPERTS)[None, None, :]).astype(jnp.float32)
    gate_prob = jax.nn.softmax(jnp.sum(onehot * logits[:, None, :], axis=-1), axis=-1)
    gate_mat = jnp.sum(gate_prob[:, :, None] * onehot, axis=1)
    gate_act = jnp.einsum('bd,edf->bef', normed_mid.astype(jnp.float32), w_gate.astype(jnp.float32))
    up_act = jnp.einsum('bd,edf->bef', normed_mid.astype(jnp.float32), w_up.astype(jnp.float32))
    expert_in = (jax.nn.silu(gate_act) * up_act * gate_mat[:, :, None]).astype(jnp.bfloat16)
    moe_out = jnp.einsum('bef,efd->bd', expert_in.astype(jnp.float32), w_down.astype(jnp.float32))
    return (x_mid.astype(jnp.float32) + moe_out).astype(jnp.bfloat16), key_cache, val_cache


def reference(hidden, lengths, choice, keys_one, vals_one, keys_two, vals_two, g_attn, w_q, w_k, w_v, w_o, g_mlp, w_router, w_gate, w_up, w_down):
    caches = [(keys_one, vals_one), (keys_two, vals_two)]
    results = []
    for layer_idx in range(LAYERS):
        hidden, key_cache, val_cache = decode_layer(hidden, lengths, choice[layer_idx], caches[layer_idx][0], caches[layer_idx][1], g_attn[layer_idx], w_q[layer_idx], w_k[layer_idx], w_v[layer_idx], w_o[layer_idx], g_mlp[layer_idx], w_router[layer_idx], w_gate[layer_idx], w_up[layer_idx], w_down[layer_idx])
        results.append(key_cache)
        results.append(val_cache)
    return (hidden, results[0], results[1], results[2], results[3])
```

```python
import jax
import jax.numpy as jnp
import numpy as np
from jax import lax
from jax.experimental import pallas as pl
from jax.experimental.pallas import tpu as pltpu
from jax.sharding import PartitionSpec as P

EPS = 1e-5
THETA = 1000000.0
N = 8
B = 32
D = 1536
SEQ = 128
CH = 4
QUADS = 10
NT = (((1,), (1,)), ((), ()))
PEERS = ((1, 1, 0), (1, 0, 1), (0, 1, 0), (1, 1, 1), (1, 0, 0), (0, 1, 1), (0, 0, 1))


def rope_tables():
    half = 32
    inv = np.power(np.float32(THETA), (-2.0 * np.arange(half, dtype=np.float32) / 64).astype(np.float32)).astype(np.float32)
    angle = (np.arange(SEQ, dtype=np.float32)[:, None] * inv[None, :]).astype(np.float32).astype(np.float64)
    cos = np.tile(np.cos(angle), (1, 4)).astype(np.float32)
    sin = np.tile(np.sin(angle), (1, 4)).astype(np.float32)
    return cos, sin


def dot_nt(a, b):
    return lax.dot_general(a, b, NT, preferred_element_type=jnp.float32)


def dot_nn(a, b):
    return jnp.dot(a, b, preferred_element_type=jnp.float32)


def kernel(len_s, hid_h, choice_h, k1_h, v1_h, k2_h, v2_h, ga_h, wq_h, wk_h, wv_h, wo_h, gm_h, wr_h, wg_h, wu_h, wd_h, cos_h, sin_h,
           hid_o, kv1_o, kv2_o,
           wg, wu, wd, wqkv, wo, wr, xk, xv, stage, send, recv, outs, hb, psend, rsb, m_s, qs, sc, os_, kvn, cos_t, sin_t, cos_b, sin_b, choice_v, ga, gm, mask_s, gx, act, acc,
           s_in, s_w, s_small, s_out, a2a_ss, a2a_rs, rs_ss, rs_rs, ag_ss, ag_rs):
    me = lax.axis_index('tp')
    my, mx, mc = me // 4, (me // 2) % 2, me % 2
    peers = []
    for dy, dx, dc in PEERS:
        peers.append(((my + dy) % 2) * 4 + ((mx + dx) % 2) * 2 + (mc + dc) % 2)

    def dev(t):
        return {'tp': t}

    barrier = pltpu.get_barrier_semaphore()
    for t in peers:
        pl.semaphore_signal(barrier, inc=1, device_id=dev(t), device_id_type=pl.DeviceIdType.MESH)

    caches = ((k1_h, v1_h), (k2_h, v2_h))
    cache_cp = {}
    for l in range(2):
        for c in range(CH):
            for i, buf in enumerate((xk, xv)):
                rows = pl.ds(c * 128, 128)
                cp = pltpu.make_async_copy(caches[l][i].at[rows], buf.at[l, rows], s_in.at[l, c, i])
                cache_cp[l, c, i] = cp

    small = [
        (cos_h, cos_t), (sin_h, sin_t), (choice_h, choice_v), (ga_h, ga), (gm_h, gm), (wr_h, wr), (wo_h, wo),
    ]
    for l in range(2):
        small.append((wq_h.at[l, pl.ds(0, 128)], wqkv.at[l, pl.ds(0, 128)]))
        small.append((wk_h.at[l], wqkv.at[l, pl.ds(128, 64)]))
        small.append((wq_h.at[l, pl.ds(128, 64)], wqkv.at[l, pl.ds(192, 64)]))
        small.append((wv_h.at[l], wqkv.at[l, pl.ds(320, 64)]))
    for j in range(N):
        small.append((hid_h.at[pl.ds(16 * (j // 4), 16), pl.ds(384 * (j % 4), 384)], hb.at[0, j]))
    small_cp = [pltpu.make_async_copy(src, dst, s_small.at[i]) for i, (src, dst) in enumerate(small)]

    for c in range(CH):
        cache_cp[0, c, 0].start()
        cache_cp[0, c, 1].start()
    for cp in small_cp:
        cp.start()
    for c in range(CH):
        cache_cp[1, c, 0].start()
        cache_cp[1, c, 1].start()

    def weight_copies(l, j):
        rows = pl.ds(pl.multiple_of(j * 256, 256), 256)
        return [pltpu.make_async_copy(src.at[l, rows], dst.at[l, rows], s_w.at[l, j, i])
                for i, (src, dst) in enumerate(((wg_h, wg), (wu_h, wu), (wd_h, wd)))]

    for l in range(2):
        def start_weights(j, _, l=l):
            for cp in weight_copies(l, j):
                cp.start()
            return 0
        lax.fori_loop(0, QUADS, start_weights, 0)

    def prep(l, c):
        cache_cp[l, c, 0].wait()
        cache_cp[l, c, 1].wait()
        for i in range(2):
            rows = pl.ds(c * 128 + i * 64, 64)
            kk = xk[l, rows].astype(jnp.float32)
            vv = xv[l, rows].astype(jnp.float32)
            stage[pl.ds(i * 512, 512), :] = jnp.concatenate([kk, vv], axis=-1).reshape(512, 128)
        for h in range(N):
            send[l, c, h] = stage[pl.ds(h, 128, stride=8), :].astype(jnp.bfloat16).reshape(8, 16, 128)

    def a2a_copy(l, c, d):
        t = peers[d]
        return pltpu.make_async_remote_copy(
            src_ref=send.at[l, c, t], dst_ref=recv.at[l, c, me],
            send_sem=a2a_ss.at[l, c, d], recv_sem=a2a_rs.at[l, c, d],
            device_id=dev(t), device_id_type=pl.DeviceIdType.MESH)

    def a2a_send(l, c):
        for d in range(N - 1):
            a2a_copy(l, c, d).start()
        recv[l, c, me] = send[l, c, me]

    def a2a_wait(l, c):
        for d in range(N - 1):
            a2a_copy(l, c, d).wait_recv()

    prep(0, 0)
    pl.semaphore_wait(barrier, N - 1)
    a2a_send(0, 0)
    for c in range(1, CH):
        prep(0, c)
        a2a_send(0, c)

    for cp in small_cp:
        cp.wait()
    for l in range(2):
        wqkv[l, pl.ds(256, 64), :] = jnp.zeros((64, D), jnp.bfloat16)
    qs[...] = jnp.zeros_like(qs)

    def rope_rows(b, _):
        pos = len_s[b]
        cos_b[pl.ds(b, 1), :] = cos_t[pl.ds(pos, 1), :]
        sin_b[pl.ds(b, 1), :] = sin_t[pl.ds(pos, 1), :]
        return 0
    lax.fori_loop(0, B, rope_rows, 0)

    for l in range(2):
        ids = lax.broadcasted_iota(jnp.int32, (128, B), 0)
        picked = jnp.zeros((128, B), jnp.float32)
        for k in range(8):
            picked = jnp.where(ids == choice_v[l, pl.ds(k, 1), :], 1.0, picked)
        mask_s[l] = picked.T

    lane = lax.broadcasted_iota(jnp.int32, (B, 128), 1)
    left = lane < 64
    lower = (lane % 64) < 32

    def norm_into(src, gain_ref, l):
        for hf in range(2):
            xs = [hb[src, 4 * hf + c].astype(jnp.float32) for c in range(4)]
            sq = xs[0] * xs[0]
            for x in xs[1:]:
                sq = sq + x * x
            scale = lax.rsqrt(jnp.sum(sq, axis=-1, keepdims=True) * (1.0 / D) + EPS)
            for c in range(4):
                g = gain_ref[pl.ds(l, 1), pl.ds(384 * c, 384)].astype(jnp.float32)
                m_s[pl.ds(16 * hf, 16), pl.ds(384 * c, 384)] = (xs[c] * scale * g).astype(jnp.bfloat16)

    def rope(x):
        rot = jnp.where(lower, -pltpu.roll(x, 96, 1), pltpu.roll(x, 32, 1))
        return x * cos_b[...] + rot * sin_b[...]

    def rounded(x):
        return x.astype(jnp.bfloat16).astype(jnp.float32)

    def project(l, src):
        norm_into(src, ga, l)
        qkv = dot_nt(m_s[...], wqkv[l])
        qa = rounded(rope(qkv[:, 0:128]))
        kq = rounded(rope(qkv[:, 128:256]))
        zero = jnp.zeros_like(qa)
        qs[pl.ds(0, B, stride=8), :] = jnp.where(left, qa, zero)
        qs[pl.ds(1, B, stride=8), :] = jnp.where(left, pltpu.roll(qa, 64, 1), zero)
        qs[pl.ds(2, B, stride=8), :] = jnp.where(left, pltpu.roll(kq, 64, 1), zero)
        kvn[...] = jnp.where(left, kq, rounded(qkv[:, 256:384]))

    row_ids = lax.broadcasted_iota(jnp.int32, (SEQ, 128), 0)
    lane8 = lax.broadcasted_iota(jnp.int32, (8, 128), 1)

    def attend(l):
        def chunk(c, _):
            a2a_wait(l, c)
            tiles, scores = [], []
            for i in range(8):
                b = c * 8 + i
                pos = len_s[b]
                tile = recv[l, c, :, i].reshape(SEQ, 128).astype(jnp.float32)
                tile = jnp.where(row_ids == pos, kvn[pl.ds(b, 1), :], tile).astype(jnp.bfloat16)
                recv[l, c, :, i] = tile.reshape(8, 16, 128)
                q = qs[pl.ds(pl.multiple_of(b * 8, 8), 8), :].astype(jnp.bfloat16)
                scores.append(jnp.where(lane8 <= pos, dot_nt(q, tile) * 0.125, -1e30))
                tiles.append(tile)
            s = jnp.concatenate(scores, axis=0)
            e = jnp.exp(s - jnp.max(s, axis=-1, keepdims=True))
            p = e / jnp.sum(e, axis=-1, keepdims=True)
            for i in range(8):
                b = c * 8 + i
                o = dot_nn(p[8 * i:8 * i + 8].astype(jnp.bfloat16), tiles[i])
                os_[pl.ds(pl.multiple_of(b * 8, 8), 8), :] = o
            return 0
        lax.fori_loop(0, CH, chunk, 0)

    def attn_out(l, ar):
        o0 = os_[pl.ds(0, B, stride=8), :]
        o1 = os_[pl.ds(1, B, stride=8), :]
        o2 = os_[pl.ds(2, B, stride=8), :]
        oa = jnp.where(left, pltpu.roll(o0, 64, 1), o1).astype(jnp.bfloat16)
        ob = pltpu.roll(o2, 64, 1)[:, 0:64].astype(jnp.bfloat16)
        part = dot_nn(oa, wo[l, pl.ds(0, 128)]) + dot_nn(ob, wo[l, pl.ds(128, 64)])
        put_partial(ar, part)

    def put_partial(ar, part):
        for j in range(N):
            psend[ar, j] = part[16 * (j // 4):16 * (j // 4) + 16, 384 * (j % 4):384 * (j % 4) + 384].astype(jnp.bfloat16)

    def rs_copy(ar, d):
        t = peers[d]
        return pltpu.make_async_remote_copy(
            src_ref=psend.at[ar, t], dst_ref=rsb.at[ar, d],
            send_sem=rs_ss.at[ar, d], recv_sem=rs_rs.at[ar, d],
            device_id=dev(t), device_id_type=pl.DeviceIdType.MESH)

    def ag_copy(ar, d):
        t = peers[d]
        return pltpu.make_async_remote_copy(
            src_ref=hb.at[ar + 1, me], dst_ref=hb.at[ar + 1, me],
            send_sem=ag_ss.at[ar, d], recv_sem=ag_rs.at[ar, d],
            device_id=dev(t), device_id_type=pl.DeviceIdType.MESH)

    def reduce_all(ar, filler=None):
        for d in range(N - 1):
            rs_copy(ar, d).start()
        if filler is not None:
            filler()
        total = psend[ar, me].astype(jnp.float32)
        for d in reversed(range(N - 1)):
            rs_copy(ar, d).wait_recv()
            total = total + rsb[ar, d].astype(jnp.float32)
        hb[ar + 1, me] = (hb[ar, me].astype(jnp.float32) + total).astype(jnp.bfloat16)
        for d in range(N - 1):
            ag_copy(ar, d).start()

    def gather_wait(ar):
        for d in range(N - 1):
            ag_copy(ar, d).wait_recv()

    out_refs = (kv1_o, kv2_o)

    def out_copy(l, c):
        return pltpu.make_async_copy(outs.at[l, pl.ds(c * 8, 8)], out_refs[l].at[pl.ds(c * 8, 8)], s_out.at[l, c])

    def write_caches(l):
        def chunk(c, _):
            for i in range(8):
                outs[l, c * 8 + i] = recv[l, c, :, i].reshape(SEQ, 128).T
            out_copy(l, c).start()
            return 0
        lax.fori_loop(0, CH, chunk, 0)

    lane_w = lax.broadcasted_iota(jnp.int32, (B, 128), 1) < 64

    def experts(l, ar):
        norm_into(ar, gm, l)
        logits = dot_nt(m_s[...], wr[l])
        chosen = mask_s[l][:, 0:40] > 0.5
        top = jnp.max(jnp.where(chosen, logits, -jnp.inf), axis=-1, keepdims=True)
        e = jnp.where(chosen, jnp.exp(jnp.where(chosen, logits - top, 0.0)), 0.0)
        gate = e / jnp.sum(e, axis=-1, keepdims=True)
        for j in range(QUADS):
            for i in range(2):
                k = 4 * j + 2 * i
                g0 = jnp.broadcast_to(gate[:, k:k + 1], (B, 128))
                g1 = jnp.broadcast_to(gate[:, k + 1:k + 2], (B, 128))
                gx[j, :, pl.ds(128 * i, 128)] = jnp.where(lane_w, g0, g1)

        def up(j):
            rows = pl.ds(pl.multiple_of(j * 256, 256), 256)
            cps = weight_copies(l, j)
            for cp in cps:
                cp.wait()
            g = dot_nt(m_s[...], wg[l, rows, :])
            u = dot_nt(m_s[...], wu[l, rows, :])
            act[j] = (gx[j] * (g * jax.nn.sigmoid(g)) * u).astype(jnp.bfloat16)

        def down(j):
            rows = pl.ds(pl.multiple_of(j * 256, 256), 256)
            return dot_nn(act[j], wd[l, rows, :])

        acc[...] = jnp.zeros_like(acc)
        up(0)

        def step(j, _):
            up(j)
            acc[...] += down(j - 1)
            return 0
        lax.fori_loop(1, QUADS, step, 0)
        put_partial(ar, acc[...] + down(QUADS - 1))

    prep(1, 0)
    a2a_send(1, 0)
    project(0, 0)
    for c in range(1, CH):
        prep(1, c)
    attend(0)
    attn_out(0, 0)
    reduce_all(0, lambda: write_caches(0))
    gather_wait(0)
    for c in range(1, CH):
        a2a_send(1, c)
    experts(0, 1)
    reduce_all(1)
    gather_wait(1)
    project(1, 2)
    attend(1)
    attn_out(1, 2)
    reduce_all(2, lambda: write_caches(1))
    gather_wait(2)
    experts(1, 3)
    reduce_all(3)
    gather_wait(3)

    hid_cp = [pltpu.make_async_copy(hb.at[4, j], hid_o.at[pl.ds(16 * (j // 4), 16), pl.ds(384 * (j % 4), 384)], s_small.at[j]) for j in range(N)]
    for cp in hid_cp:
        cp.start()
    for l in range(2):
        for c in range(CH):
            out_copy(l, c).wait()
            for d in range(N - 1):
                a2a_copy(l, c, d).wait_send()
    for ar in range(4):
        for d in range(N - 1):
            rs_copy(ar, d).wait_send()
            ag_copy(ar, d).wait_send()
    for cp in hid_cp:
        cp.wait()


def solution(mesh):
    seq_spec = P('dp', 'tp', None, None)
    head_spec = P('dp', None, 'tp', None)
    col_spec = P(None, None, 'tp')
    ff_spec = P(None, None, None, 'tp')
    cos, sin = rope_tables()

    def local_step(hidden, lengths, choice, keys_one, vals_one, keys_two, vals_two, g_attn, w_q, w_k, w_v, w_o, g_mlp, w_router, w_gate, w_up, w_down):
        bf, f32 = jnp.bfloat16, jnp.float32
        any_spec = pl.BlockSpec(memory_space=pl.ANY)
        dma = pltpu.SemaphoreType.DMA
        vm = pltpu.VMEM
        operands = (
            lengths, hidden, jnp.swapaxes(choice, 1, 2),
            keys_one.reshape(512, 8, 64), vals_one.reshape(512, 8, 64), keys_two.reshape(512, 8, 64), vals_two.reshape(512, 8, 64),
            g_attn, jnp.swapaxes(w_q, 1, 2), jnp.swapaxes(w_k, 1, 2), jnp.swapaxes(w_v, 1, 2), w_o, g_mlp, jnp.swapaxes(w_router, 1, 2),
            jnp.swapaxes(w_gate, 2, 3).reshape(2, 2560, D), jnp.swapaxes(w_up, 2, 3).reshape(2, 2560, D), w_down.reshape(2, 2560, D),
            jnp.asarray(cos), jnp.asarray(sin),
        )
        hid, kv1, kv2 = pl.pallas_call(
            kernel,
            name='decode_two',
            out_shape=[jax.ShapeDtypeStruct((B, D), bf), jax.ShapeDtypeStruct((B, 128, 128), bf), jax.ShapeDtypeStruct((B, 128, 128), bf)],
            in_specs=[pl.BlockSpec(memory_space=pltpu.SMEM)] + [any_spec] * 18,
            out_specs=[any_spec] * 3,
            scratch_shapes=[
                vm((2, 2560, D), bf), vm((2, 2560, D), bf), vm((2, 2560, D), bf),
                vm((2, 384, D), bf), vm((2, 192, D), bf), vm((2, 40, D), bf),
                vm((2, 512, 8, 64), bf), vm((2, 512, 8, 64), bf), vm((1024, 128), f32),
                vm((2, CH, 8, 8, 16, 128), bf), vm((2, CH, 8, 8, 16, 128), bf), vm((2, B, 128, 128), bf),
                vm((5, 8, 16, 384), bf), vm((4, 8, 16, 384), bf), vm((4, 7, 16, 384), bf),
                vm((B, D), bf), vm((256, 128), f32), vm((8, 128), f32), vm((256, 128), f32), vm((B, 128), f32),
                vm((128, 128), f32), vm((128, 128), f32), vm((B, 128), f32), vm((B, 128), f32),
                vm((2, 8, B), jnp.int32), vm((2, D), bf), vm((2, D), bf),
                vm((2, B, 128), f32), vm((QUADS, B, 256), f32), vm((QUADS, B, 256), bf), vm((B, D), f32),
                dma((2, CH, 2)), dma((2, QUADS, 3)), dma((23,)), dma((2, CH)),
                dma((2, CH, 7)), dma((2, CH, 7)), dma((4, 7)), dma((4, 7)), dma((4, 7)), dma((4, 7)),
            ],
            compiler_params=pltpu.CompilerParams(collective_id=0, has_side_effects=True, vmem_limit_bytes=67043328),
        )(*operands)
        outs = []
        for kv in (kv1, kv2):
            outs.append(jnp.swapaxes(kv[:, 0:64], 1, 2)[:, :, None, :])
            outs.append(jnp.swapaxes(kv[:, 64:128], 1, 2)[:, :, None, :])
        return (hid, outs[0], outs[1], outs[2], outs[3])

    return jax.shard_map(local_step, mesh=mesh, in_specs=(P('dp', None), P('dp'), P(None, 'dp', None), seq_spec, seq_spec, seq_spec, seq_spec, P(), col_spec, col_spec, col_spec, P(None, 'tp', None), P(), P(), ff_spec, ff_spec, P(None, None, 'tp', None)), out_specs=(P('dp', None), head_spec, head_spec, head_spec, head_spec), check_vma=False)
```

```python
import jax
import jax.numpy as jnp
import numpy as np
from jax import lax
from jax.experimental import pallas as pl
from jax.experimental.pallas import tpu as pltpu
from jax.sharding import PartitionSpec as P

EPS = 1e-5
THETA = 1000000.0
N = 8
B = 32
D = 1536
SEQ = 128
CH = 4
QUADS = 10
NT = (((1,), (1,)), ((), ()))
PEERS = ((1, 1, 0), (1, 0, 1), (0, 1, 0), (1, 1, 1), (1, 0, 0), (0, 1, 1), (0, 0, 1))


def rope_tables():
    half = 32
    inv = np.power(np.float32(THETA), (-2.0 * np.arange(half, dtype=np.float32) / 64).astype(np.float32)).astype(np.float32)
    angle = (np.arange(SEQ, dtype=np.float32)[:, None] * inv[None, :]).astype(np.float32).astype(np.float64)
    cos = np.tile(np.cos(angle), (1, 4)).astype(np.float32)
    sin = np.tile(np.sin(angle), (1, 4)).astype(np.float32)
    return cos, sin


def dot_nt(a, b):
    return lax.dot_general(a, b, NT, preferred_element_type=jnp.float32)


def dot_nn(a, b):
    return jnp.dot(a, b, preferred_element_type=jnp.float32)


def kernel(len_s, hid_h, choice_h, k1_h, v1_h, k2_h, v2_h, ga_h, wq_h, wk_h, wv_h, wo_h, gm_h, wr_h, wg_h, wu_h, wd_h, cos_h, sin_h,
           hid_o, outs1, outs2,
           wg, wu, wd, wqkv, wo, wr, xk, xv, stage, send, recv, hb, psend, rsb, m_s, qs, sc, os_, kvn, cos_t, sin_t, cos_b, sin_b, choice_v, ga, gm, mask_s, gx, act, acc,
           s_in, s_w, s_small, a2a_ss, a2a_rs, ar_ss, rs_rs, ag_rs):
    me = lax.axis_index('tp')
    my, mx, mc = me // 4, (me // 2) % 2, me % 2
    peers = []
    for dy, dx, dc in PEERS:
        peers.append(((my + dy) % 2) * 4 + ((mx + dx) % 2) * 2 + (mc + dc) % 2)

    def dev(t):
        return {'tp': t}

    def landed(like, sem):
        pltpu.make_async_copy(like, like, sem).wait()

    barrier = pltpu.get_barrier_semaphore()
    for t in peers:
        pl.semaphore_signal(barrier, inc=1, device_id=dev(t), device_id_type=pl.DeviceIdType.MESH)

    caches = ((k1_h, v1_h), (k2_h, v2_h))
    cache_cp = {}
    for l in range(2):
        for c in range(CH):
            for i, buf in enumerate((xk, xv)):
                rows = pl.ds(c * 128, 128)
                cp = pltpu.make_async_copy(caches[l][i].at[rows], buf.at[l, rows], s_in.at[l, c])
                cache_cp[l, c, i] = cp

    small = [
        (cos_h, cos_t), (sin_h, sin_t), (choice_h, choice_v), (ga_h, ga), (gm_h, gm), (wr_h, wr), (wo_h, wo),
    ]
    for l in range(2):
        small.append((wq_h.at[l, pl.ds(0, 128)], wqkv.at[l, pl.ds(0, 128)]))
        small.append((wk_h.at[l], wqkv.at[l, pl.ds(128, 64)]))
        small.append((wq_h.at[l, pl.ds(128, 64)], wqkv.at[l, pl.ds(192, 64)]))
        small.append((wv_h.at[l], wqkv.at[l, pl.ds(320, 64)]))
    for j in range(N):
        small.append((hid_h.at[pl.ds(16 * (j // 4), 16), pl.ds(384 * (j % 4), 384)], hb.at[0, j]))
    small_cp = [pltpu.make_async_copy(src, dst, s_small) for src, dst in small]

    for c in range(CH):
        cache_cp[0, c, 0].start()
        cache_cp[0, c, 1].start()
    for cp in small_cp:
        cp.start()
    for c in range(CH):
        cache_cp[1, c, 0].start()
        cache_cp[1, c, 1].start()

    def weight_copies(l, j):
        rows = pl.ds(pl.multiple_of(j * 256, 256), 256)
        return [pltpu.make_async_copy(src.at[l, rows], dst.at[l, rows], s_w.at[l, j])
                for src, dst in ((wg_h, wg), (wu_h, wu), (wd_h, wd))]

    for l in range(2):
        def start_weights(j, _, l=l):
            for cp in weight_copies(l, j):
                cp.start()
            return 0
        lax.fori_loop(0, QUADS, start_weights, 0)

    def prep(l, c):
        landed(xk.at[l, pl.ds(0, 256)], s_in.at[l, c])
        for i in range(2):
            rows = pl.ds(c * 128 + i * 64, 64)
            kk = xk[l, rows].astype(jnp.float32)
            vv = xv[l, rows].astype(jnp.float32)
            stage[pl.ds(i * 512, 512), :] = jnp.concatenate([kk, vv], axis=-1).reshape(512, 128)
        for h in range(N):
            send[l, c, h] = stage[pl.ds(h, 128, stride=8), :].astype(jnp.bfloat16).reshape(8, 16, 128)

    def a2a_copy(l, c, d):
        t = peers[d]
        return pltpu.make_async_remote_copy(
            src_ref=send.at[l, c, t], dst_ref=recv.at[l, c, me],
            send_sem=a2a_ss, recv_sem=a2a_rs.at[l, c],
            device_id=dev(t), device_id_type=pl.DeviceIdType.MESH)

    def a2a_send(l, c):
        for d in range(N - 1):
            a2a_copy(l, c, d).start()
        recv[l, c, me] = send[l, c, me]

    def a2a_wait(l, c):
        landed(recv.at[l, c, pl.ds(0, N - 1)], a2a_rs.at[l, c])

    prep(0, 0)
    pl.semaphore_wait(barrier, N - 1)
    a2a_send(0, 0)
    for c in range(1, CH):
        prep(0, c)
        a2a_send(0, c)

    for cp in small_cp:
        cp.wait()
    for l in range(2):
        wqkv[l, pl.ds(256, 64), :] = jnp.zeros((64, D), jnp.bfloat16)
    qs[...] = jnp.zeros_like(qs)

    def rope_rows(b, _):
        pos = len_s[b]
        cos_b[pl.ds(b, 1), :] = cos_t[pl.ds(pos, 1), :]
        sin_b[pl.ds(b, 1), :] = sin_t[pl.ds(pos, 1), :]
        return 0
    lax.fori_loop(0, B, rope_rows, 0)

    for l in range(2):
        ids = lax.broadcasted_iota(jnp.int32, (128, B), 0)
        picked = jnp.zeros((128, B), jnp.float32)
        for k in range(8):
            picked = jnp.where(ids == choice_v[l, pl.ds(k, 1), :], 1.0, picked)
        mask_s[l] = picked.T

    lane = lax.broadcasted_iota(jnp.int32, (B, 128), 1)
    left = lane < 64
    lower = (lane % 64) < 32

    def norm_into(src, gain_ref, l):
        for hf in range(2):
            xs = [hb[src, 4 * hf + c].astype(jnp.float32) for c in range(4)]
            sq = xs[0] * xs[0]
            for x in xs[1:]:
                sq = sq + x * x
            scale = lax.rsqrt(jnp.sum(sq, axis=-1, keepdims=True) * (1.0 / D) + EPS)
            for c in range(4):
                g = gain_ref[pl.ds(l, 1), pl.ds(384 * c, 384)].astype(jnp.float32)
                m_s[pl.ds(16 * hf, 16), pl.ds(384 * c, 384)] = (xs[c] * scale * g).astype(jnp.bfloat16)

    def rope(x):
        rot = jnp.where(lower, -pltpu.roll(x, 96, 1), pltpu.roll(x, 32, 1))
        return x * cos_b[...] + rot * sin_b[...]

    def rounded(x):
        return x.astype(jnp.bfloat16).astype(jnp.float32)

    def project(l, src):
        norm_into(src, ga, l)
        qkv = dot_nt(m_s[...], wqkv[l])
        qa = rounded(rope(qkv[:, 0:128]))
        kq = rounded(rope(qkv[:, 128:256]))
        zero = jnp.zeros_like(qa)
        qs[pl.ds(0, B, stride=8), :] = jnp.where(left, qa, zero)
        qs[pl.ds(1, B, stride=8), :] = jnp.where(left, pltpu.roll(qa, 64, 1), zero)
        qs[pl.ds(2, B, stride=8), :] = jnp.where(left, pltpu.roll(kq, 64, 1), zero)
        kvn[...] = jnp.where(left, kq, rounded(qkv[:, 256:384]))

    row_ids = lax.broadcasted_iota(jnp.int32, (SEQ, 128), 0)
    lane8 = lax.broadcasted_iota(jnp.int32, (8, 128), 1)

    def attend(l):
        def chunk(c, _):
            a2a_wait(l, c)
            tiles, scores = [], []
            for i in range(8):
                b = c * 8 + i
                pos = len_s[b]
                tile = recv[l, c, :, i].reshape(SEQ, 128).astype(jnp.float32)
                tile = jnp.where(row_ids == pos, kvn[pl.ds(b, 1), :], tile).astype(jnp.bfloat16)
                recv[l, c, :, i] = tile.reshape(8, 16, 128)
                q = qs[pl.ds(pl.multiple_of(b * 8, 8), 8), :].astype(jnp.bfloat16)
                scores.append(jnp.where(lane8 <= pos, dot_nt(q, tile) * 0.125, -1e30))
                tiles.append(tile)
            s = jnp.concatenate(scores, axis=0)
            e = jnp.exp(s - jnp.max(s, axis=-1, keepdims=True))
            p = e / jnp.sum(e, axis=-1, keepdims=True)
            for i in range(8):
                b = c * 8 + i
                o = dot_nn(p[8 * i:8 * i + 8].astype(jnp.bfloat16), tiles[i])
                os_[pl.ds(pl.multiple_of(b * 8, 8), 8), :] = o
            return 0
        lax.fori_loop(0, CH, chunk, 0)

    def attn_out(l, ar):
        o0 = os_[pl.ds(0, B, stride=8), :]
        o1 = os_[pl.ds(1, B, stride=8), :]
        o2 = os_[pl.ds(2, B, stride=8), :]
        oa = jnp.where(left, pltpu.roll(o0, 64, 1), o1).astype(jnp.bfloat16)
        ob = pltpu.roll(o2, 64, 1)[:, 0:64].astype(jnp.bfloat16)
        part = dot_nn(oa, wo[l, pl.ds(0, 128)]) + dot_nn(ob, wo[l, pl.ds(128, 64)])
        put_partial(ar, part)

    def put_partial(ar, part):
        for j in range(N):
            psend[ar, j] = part[16 * (j // 4):16 * (j // 4) + 16, 384 * (j % 4):384 * (j % 4) + 384].astype(jnp.bfloat16)

    def rs_copy(ar, d):
        t = peers[d]
        return pltpu.make_async_remote_copy(
            src_ref=psend.at[ar, t], dst_ref=rsb.at[ar, d],
            send_sem=ar_ss, recv_sem=rs_rs.at[ar],
            device_id=dev(t), device_id_type=pl.DeviceIdType.MESH)

    def ag_copy(ar, d):
        t = peers[d]
        return pltpu.make_async_remote_copy(
            src_ref=hb.at[ar + 1, me], dst_ref=hb.at[ar + 1, me],
            send_sem=ar_ss, recv_sem=ag_rs.at[ar],
            device_id=dev(t), device_id_type=pl.DeviceIdType.MESH)

    def reduce_all(ar, filler=None):
        for d in range(N - 1):
            rs_copy(ar, d).start()
        if filler is not None:
            filler()
        total = psend[ar, me].astype(jnp.float32)
        landed(rsb.at[ar], rs_rs.at[ar])
        for d in range(N - 1):
            total = total + rsb[ar, d].astype(jnp.float32)
        hb[ar + 1, me] = (hb[ar, me].astype(jnp.float32) + total).astype(jnp.bfloat16)
        for d in range(N - 1):
            ag_copy(ar, d).start()

    def gather_wait(ar):
        landed(rsb.at[ar], ag_rs.at[ar])

    out_refs = (outs1, outs2)

    def write_caches(l):
        def chunk(c, _):
            for i in range(8):
                out_refs[l][c * 8 + i] = recv[l, c, :, i].reshape(SEQ, 128).T
            return 0
        lax.fori_loop(0, CH, chunk, 0)

    lane_w = lax.broadcasted_iota(jnp.int32, (B, 128), 1) < 64

    def experts(l, ar):
        norm_into(ar, gm, l)
        logits = dot_nt(m_s[...], wr[l])
        chosen = mask_s[l][:, 0:40] > 0.5
        top = jnp.max(jnp.where(chosen, logits, -jnp.inf), axis=-1, keepdims=True)
        e = jnp.where(chosen, jnp.exp(jnp.where(chosen, logits - top, 0.0)), 0.0)
        gate = e / jnp.sum(e, axis=-1, keepdims=True)
        for j in range(QUADS):
            for i in range(2):
                k = 4 * j + 2 * i
                g0 = jnp.broadcast_to(gate[:, k:k + 1], (B, 128))
                g1 = jnp.broadcast_to(gate[:, k + 1:k + 2], (B, 128))
                gx[j, :, pl.ds(128 * i, 128)] = jnp.where(lane_w, g0, g1)

        def up(j):
            rows = pl.ds(pl.multiple_of(j * 256, 256), 256)
            landed(wg.at[l, pl.ds(0, 768)], s_w.at[l, j])
            g = dot_nt(m_s[...], wg[l, rows, :])
            u = dot_nt(m_s[...], wu[l, rows, :])
            act[j] = (gx[j] * (g * jax.nn.sigmoid(g)) * u).astype(jnp.bfloat16)

        def down(j):
            rows = pl.ds(pl.multiple_of(j * 256, 256), 256)
            return dot_nn(act[j], wd[l, rows, :])

        acc[...] = jnp.zeros_like(acc)
        up(0)

        def step(j, _):
            up(j)
            acc[...] += down(j - 1)
            return 0
        lax.fori_loop(1, QUADS, step, 0)
        put_partial(ar, acc[...] + down(QUADS - 1))

    SC = jax.named_scope
    with SC("p_prep1"):
        prep(1, 0)
        a2a_send(1, 0)
    with SC("p_proj0"):
        project(0, 0)
    with SC("p_prep1b"):
        for c in range(1, CH):
            prep(1, c)
    with SC("p_att0"):
        attend(0)
    with SC("p_aout0"):
        attn_out(0, 0)
    with SC("p_rs0"):
        reduce_all(0, lambda: write_caches(0))
    with SC("p_ag0"):
        gather_wait(0)
    for c in range(1, CH):
        a2a_send(1, c)
    with SC("p_moe0"):
        experts(0, 1)
    with SC("p_rs1"):
        reduce_all(1)
    with SC("p_ag1"):
        gather_wait(1)
    with SC("p_proj1"):
        project(1, 2)
    with SC("p_att1"):
        attend(1)
    with SC("p_aout1"):
        attn_out(1, 2)
    with SC("p_rs2"):
        reduce_all(2, lambda: write_caches(1))
    with SC("p_ag2"):
        gather_wait(2)
    with SC("p_moe1"):
        experts(1, 3)
    with SC("p_rs3"):
        reduce_all(3)
    with SC("p_ag3"):
        gather_wait(3)

    with SC("p_end"):
        for j in range(N):
            hid_o[pl.ds(16 * (j // 4), 16), pl.ds(384 * (j % 4), 384)] = hb[4, j]
        landed(send.at[:, :, pl.ds(0, N - 1)], a2a_ss)
        landed(rsb, ar_ss)
        landed(rsb, ar_ss)


def tail_kernel(hid, kv1, kv2, hid_o, k1_o, v1_o, k2_o, v2_o, sem):
    copies = [
        (kv1.at[:, pl.ds(0, 64)], k1_o), (kv1.at[:, pl.ds(64, 64)], v1_o),
        (kv2.at[:, pl.ds(0, 64)], k2_o), (kv2.at[:, pl.ds(64, 64)], v2_o),
        (hid, hid_o),
    ]
    cps = [pltpu.make_async_copy(src, dst, sem.at[i]) for i, (src, dst) in enumerate(copies)]
    for cp in cps:
        cp.start()
    for cp in cps:
        cp.wait()


def solution(mesh):
    seq_spec = P('dp', 'tp', None, None)
    head_spec = P('dp', None, 'tp', None)
    col_spec = P(None, None, 'tp')
    ff_spec = P(None, None, None, 'tp')
    cos, sin = rope_tables()

    def local_step(hidden, lengths, choice, keys_one, vals_one, keys_two, vals_two, g_attn, w_q, w_k, w_v, w_o, g_mlp, w_router, w_gate, w_up, w_down):
        bf, f32 = jnp.bfloat16, jnp.float32
        any_spec = pl.BlockSpec(memory_space=pl.ANY)
        vmem_spec = pl.BlockSpec(memory_space=pltpu.VMEM)
        dma = pltpu.SemaphoreType.DMA
        vm = pltpu.VMEM
        operands = (
            lengths, hidden, jnp.swapaxes(choice, 1, 2),
            keys_one.reshape(512, 8, 64), vals_one.reshape(512, 8, 64), keys_two.reshape(512, 8, 64), vals_two.reshape(512, 8, 64),
            g_attn, jnp.swapaxes(w_q, 1, 2), jnp.swapaxes(w_k, 1, 2), jnp.swapaxes(w_v, 1, 2), w_o, g_mlp, jnp.swapaxes(w_router, 1, 2),
            jnp.swapaxes(w_gate, 2, 3).reshape(2, 2560, D), jnp.swapaxes(w_up, 2, 3).reshape(2, 2560, D), w_down.reshape(2, 2560, D),
            jnp.asarray(cos), jnp.asarray(sin),
        )
        hid, kv1, kv2 = pl.pallas_call(
            kernel,
            name='decode_two',
            out_shape=[vm((B, D), bf), vm((B, 128, 128), bf), vm((B, 128, 128), bf)],
            in_specs=[pl.BlockSpec(memory_space=pltpu.SMEM)] + [any_spec] * 18,
            out_specs=[vmem_spec] * 3,
            scratch_shapes=[
                vm((2, 2560, D), bf), vm((2, 2560, D), bf), vm((2, 2560, D), bf),
                vm((2, 384, D), bf), vm((2, 192, D), bf), vm((2, 40, D), bf),
                vm((2, 512, 8, 64), bf), vm((2, 512, 8, 64), bf), vm((1024, 128), f32),
                vm((2, CH, 8, 8, 16, 128), bf), vm((2, CH, 8, 8, 16, 128), bf),
                vm((5, 8, 16, 384), bf), vm((4, 8, 16, 384), bf), vm((4, 7, 16, 384), bf),
                vm((B, D), bf), vm((256, 128), f32), vm((8, 128), f32), vm((256, 128), f32), vm((B, 128), f32),
                vm((128, 128), f32), vm((128, 128), f32), vm((B, 128), f32), vm((B, 128), f32),
                vm((2, 8, B), jnp.int32), vm((2, D), bf), vm((2, D), bf),
                vm((2, B, 128), f32), vm((QUADS, B, 256), f32), vm((QUADS, B, 256), bf), vm((B, D), f32),
                dma((2, CH)), dma((2, QUADS)), dma, dma, dma((2, CH)), dma, dma((4,)), dma((4,)),
            ],
            compiler_params=pltpu.CompilerParams(collective_id=0, has_side_effects=True, vmem_limit_bytes=63500000),
        )(*operands)
        hid_out, *caches = pl.pallas_call(
            tail_kernel,
            name='write_out',
            out_shape=[jax.ShapeDtypeStruct((B, D), bf)] + [jax.ShapeDtypeStruct((B, 64, 128), bf)] * 4,
            in_specs=[vmem_spec] * 3,
            out_specs=[any_spec] * 5,
            scratch_shapes=[dma((5,))],
            compiler_params=pltpu.CompilerParams(vmem_limit_bytes=4 << 20),
        )(hid, kv1, kv2)
        return (hid_out, *[jnp.swapaxes(kv, 1, 2)[:, :, None, :] for kv in caches])

    return jax.shard_map(local_step, mesh=mesh, in_specs=(P('dp', None), P('dp'), P(None, 'dp', None), seq_spec, seq_spec, seq_spec, seq_spec, P(), col_spec, col_spec, col_spec, P(None, 'tp', None), P(), P(), ff_spec, ff_spec, P(None, None, 'tp', None)), out_specs=(P('dp', None), head_spec, head_spec, head_spec, head_spec), check_vma=False)
```

```python
import jax
import jax.numpy as jnp
import numpy as np
from jax import lax
from jax.experimental import pallas as pl
from jax.experimental.pallas import tpu as pltpu
from jax.sharding import PartitionSpec as P

EPS = 1e-5
THETA = 1000000.0
N = 8
B = 32
D = 1536
SEQ = 128
LANES, HEAD, ROWS, COLS, TILE, SLOTS, WIDE = 128, 64, 16, 384, 256, 512, 768
CH = 4
TP = 8
QUADS = 10
NT = (((1,), (1,)), ((), ()))
PEERS = ((1, 1, 0), (1, 1, 1), (1, 0, 1), (0, 1, 0), (1, 0, 0), (0, 1, 1), (0, 0, 1))


def rope_tables():
    half = 32
    inv = np.power(np.float32(THETA), (-2.0 * np.arange(half, dtype=np.float32) / HEAD).astype(np.float32)).astype(np.float32)
    angle = (np.arange(SEQ, dtype=np.float32)[:, None] * inv[None, :]).astype(np.float32).astype(np.float64)
    cos = np.tile(np.cos(angle), (1, 4)).astype(np.float32)
    sin = np.tile(np.sin(angle), (1, 4)).astype(np.float32)
    return cos, sin


def dot_nt(a, b):
    return lax.dot_general(a, b, NT, preferred_element_type=jnp.float32)


def dot_nn(a, b):
    return jnp.dot(a, b, preferred_element_type=jnp.float32)


def kernel(len_s, hid_h, choice_h, k1_h, v1_h, k2_h, v2_h, ga_h, wq_h, wk_h, wv_h, wo_h, gm_h, wr_h, wg_h, wu_h, wd_h, cos_h, sin_h,
           hid_o, outs1, outs2,
           wg, wu, wd, wqkv, wo, wr, xk, xv, stage, send, recv, hb, psend, rsb, m_s, qs, sc, os_, kvn, cos_t, sin_t, cos_b, sin_b, choice_v, ga, gm, mask_s, gx, act, acts,
           s_in, s_w, s_d, s_small, a2a_ss, a2a_rs, ar_ss, rs_rs, ag_rs):
    me = lax.axis_index('tp')
    my, mx, mc = me // 4, (me // 2) % 2, me % 2
    peers = []
    for dy, dx, dc in PEERS:
        peers.append(((my + dy) % 2) * 4 + ((mx + dx) % 2) * 2 + (mc + dc) % 2)

    def dev(t):
        return {'tp': t}

    def landed(like, sem):
        pltpu.make_async_copy(like, like, sem).wait()

    caches = ((k1_h, v1_h), (k2_h, v2_h))
    cache_cp = {}
    for l in range(2):
        for c in range(CH):
            for i, buf in enumerate((xk, xv)):
                rows = pl.ds(c * LANES, LANES)
                cp = pltpu.make_async_copy(caches[l][i].at[rows], buf.at[l, rows], s_in.at[l, c])
                cache_cp[l, c, i] = cp

    for c in range(CH):
        cache_cp[0, c, 0].start()
        cache_cp[0, c, 1].start()

    barrier = pltpu.get_barrier_semaphore()
    for t in peers:
        pl.semaphore_signal(barrier, inc=1, device_id=dev(t), device_id_type=pl.DeviceIdType.MESH)

    small = [
        (cos_h, cos_t), (sin_h, sin_t), (choice_h, choice_v), (ga_h, ga), (gm_h, gm), (wr_h, wr), (wo_h, wo),
    ]
    for l in range(2):
        small.append((wq_h.at[l, pl.ds(0, LANES)], wqkv.at[l, pl.ds(0, LANES)]))
        small.append((wk_h.at[l], wqkv.at[l, pl.ds(LANES, HEAD)]))
        small.append((wq_h.at[l, pl.ds(LANES, HEAD)], wqkv.at[l, pl.ds(192, HEAD)]))
        small.append((wv_h.at[l], wqkv.at[l, pl.ds(320, HEAD)]))
    for j in range(N):
        small.append((hid_h.at[pl.ds(ROWS * (j // 4), ROWS), pl.ds(COLS * (j % 4), COLS)], hb.at[0, j]))
    small_cp = [pltpu.make_async_copy(src, dst, s_small) for src, dst in small]

    def weight_rows(j):
        return pl.ds(pl.multiple_of(j * TILE, TILE), TILE)

    def start_rest():
        for cp in small_cp:
            cp.start()
        for c in range(CH):
            cache_cp[1, c, 0].start()
            cache_cp[1, c, 1].start()
        for l in range(2):
            def start_gate_up(j, _, l=l):
                rows = weight_rows(j)
                pltpu.make_async_copy(wg_h.at[l, rows], wg.at[l, rows], s_w.at[l, j]).start()
                pltpu.make_async_copy(wu_h.at[l, rows], wu.at[l, rows], s_w.at[l, j]).start()
                return 0
            lax.fori_loop(0, QUADS, start_gate_up, 0)
            def start_down(j, _, l=l):
                rows = weight_rows(j)
                pltpu.make_async_copy(wd_h.at[l, rows], wd.at[l, rows], s_d.at[l]).start()
                return 0
            lax.fori_loop(0, QUADS, start_down, 0)

    def prep(l, c):
        landed(xk.at[l, pl.ds(0, TILE)], s_in.at[l, c])
        for i in range(2):
            rows = pl.ds(c * LANES + i * HEAD, HEAD)
            kk = xk[l, rows].astype(jnp.float32)
            vv = xv[l, rows].astype(jnp.float32)
            stage[pl.ds(i * SLOTS, SLOTS), :] = jnp.concatenate([kk, vv], axis=-1).reshape(SLOTS, LANES)
        for h in range(N):
            rows = stage[pl.ds(h, LANES, stride=8), :].astype(jnp.bfloat16).reshape(2, 4, ROWS, LANES)
            send[l, 2 * c, h] = rows[0]
            send[l, 2 * c + 1, h] = rows[1]

    def a2a_copy(l, p, d):
        t = peers[d]
        return pltpu.make_async_remote_copy(
            src_ref=send.at[l, p, t], dst_ref=recv.at[l, p, me],
            send_sem=a2a_ss, recv_sem=a2a_rs.at[l, p],
            device_id=dev(t), device_id_type=pl.DeviceIdType.MESH)

    def a2a_send2(l, p):
        for d in range(N - 1):
            t = peers[d]
            pltpu.make_async_remote_copy(
                src_ref=send.at[l, pl.ds(p, 2), t], dst_ref=recv.at[l, pl.ds(p, 2), me],
                send_sem=a2a_ss, recv_sem=a2a_rs.at[l, p],
                device_id=dev(t), device_id_type=pl.DeviceIdType.MESH).start()
        recv[l, pl.ds(p, 2), me] = send[l, pl.ds(p, 2), me]

    def a2a_send(l, p):
        for d in range(N - 1):
            a2a_copy(l, p, d).start()
        recv[l, p, me] = send[l, p, me]

    def a2a_wait(l, p):
        landed(recv.at[l, p, pl.ds(0, N - 1)], a2a_rs.at[l, p])

    with jax.named_scope('p_prep0'):
        prep(0, 0)
    with jax.named_scope('p_bar'):
        pl.semaphore_wait(barrier, N - 1)
    with jax.named_scope('p_send0'):
        a2a_send2(0, 0)
        for c in range(1, CH):
            prep(0, c)
            a2a_send2(0, 2 * c)
    with jax.named_scope('p_rest'):
        start_rest()

    for cp in small_cp:
        cp.wait()
    for l in range(2):
        wqkv[l, pl.ds(TILE, HEAD), :] = jnp.zeros((HEAD, D), jnp.bfloat16)
    qs[...] = jnp.zeros_like(qs)

    def rope_rows(b, _):
        pos = len_s[b]
        cos_b[pl.ds(b, 1), :] = cos_t[pl.ds(pos, 1), :]
        sin_b[pl.ds(b, 1), :] = sin_t[pl.ds(pos, 1), :]
        return 0
    lax.fori_loop(0, B, rope_rows, 0)

    for l in range(2):
        ids = lax.broadcasted_iota(jnp.int32, (LANES, B), 0)
        picked = jnp.zeros((LANES, B), jnp.float32)
        for k in range(8):
            picked = jnp.where(ids == choice_v[l, pl.ds(k, 1), :], 1.0, picked)
        mask_s[l] = picked.T

    lane = lax.broadcasted_iota(jnp.int32, (B, LANES), 1)
    left = lane < HEAD
    lower = (lane % HEAD) < 32

    def norm_into(src, gain_ref, l):
        for hf in range(2):
            xs = [hb[src, 4 * hf + c].astype(jnp.float32) for c in range(4)]
            sq = xs[0] * xs[0]
            for x in xs[1:]:
                sq = sq + x * x
            scale = lax.rsqrt(jnp.sum(sq, axis=-1, keepdims=True) * (1.0 / D) + EPS)
            for c in range(4):
                g = gain_ref[pl.ds(l, 1), pl.ds(COLS * c, COLS)].astype(jnp.float32)
                m_s[pl.ds(ROWS * hf, ROWS), pl.ds(COLS * c, COLS)] = (xs[c] * scale * g).astype(jnp.bfloat16)

    def rope(x):
        rot = jnp.where(lower, -pltpu.roll(x, 96, 1), pltpu.roll(x, 32, 1))
        return x * cos_b[...] + rot * sin_b[...]

    def rounded(x):
        return x.astype(jnp.bfloat16).astype(jnp.float32)

    def project(l, src):
        norm_into(src, ga, l)
        qkv = dot_nt(m_s[...], wqkv[l])
        qa = rounded(rope(qkv[:, 0:LANES]))
        kq = rounded(rope(qkv[:, LANES:TILE]))
        zero = jnp.zeros_like(qa)
        qs[pl.ds(0, B, stride=8), :] = jnp.where(left, qa, zero)
        qs[pl.ds(1, B, stride=8), :] = jnp.where(left, pltpu.roll(qa, HEAD, 1), zero)
        qs[pl.ds(2, B, stride=8), :] = jnp.where(left, pltpu.roll(kq, HEAD, 1), zero)
        kvn[...] = jnp.where(left, kq, rounded(qkv[:, TILE:COLS]))

    row_ids = lax.broadcasted_iota(jnp.int32, (SEQ, LANES), 0)
    lane8 = lax.broadcasted_iota(jnp.int32, (8, LANES), 1)

    def attend(l):
        def chunk(c, _):
            if l == 0:
                landed(recv.at[l, pl.ds(0, 2), pl.ds(0, N - 1)], a2a_rs.at[l, 2 * c])
            else:
                a2a_wait(l, 2 * c)
                a2a_wait(l, 2 * c + 1)
            tiles, scores = [], []
            for i in range(8):
                b = c * 8 + i
                pos = len_s[b]
                tile = recv[l, 2 * c + i // 4, :, i % 4].reshape(SEQ, LANES).astype(jnp.float32)
                tile = jnp.where(row_ids == pos, kvn[pl.ds(b, 1), :], tile).astype(jnp.bfloat16)
                recv[l, 2 * c + i // 4, :, i % 4] = tile.reshape(8, ROWS, LANES)
                q = qs[pl.ds(pl.multiple_of(b * 8, 8), 8), :].astype(jnp.bfloat16)
                scores.append(jnp.where(lane8 <= pos, dot_nt(q, tile) * 0.125, -1e30))
                tiles.append(tile)
            s = jnp.concatenate(scores, axis=0)
            e = jnp.exp(s - jnp.max(s, axis=-1, keepdims=True))
            p = e / jnp.sum(e, axis=-1, keepdims=True)
            for i in range(8):
                b = c * 8 + i
                o = dot_nn(p[8 * i:8 * i + 8].astype(jnp.bfloat16), tiles[i])
                os_[pl.ds(pl.multiple_of(b * 8, 8), 8), :] = o
            return 0
        lax.fori_loop(0, CH, chunk, 0)

    def attn_out(l, ar):
        o0 = os_[pl.ds(0, B, stride=8), :]
        o1 = os_[pl.ds(1, B, stride=8), :]
        o2 = os_[pl.ds(2, B, stride=8), :]
        oa = jnp.where(left, pltpu.roll(o0, HEAD, 1), o1).astype(jnp.bfloat16)
        ob = pltpu.roll(o2, HEAD, 1)[:, 0:HEAD].astype(jnp.bfloat16)
        part = dot_nn(oa, wo[l, pl.ds(0, LANES)]) + dot_nn(ob, wo[l, pl.ds(LANES, HEAD)])
        put_partial(ar, part)

    def put_partial(ar, part):
        for j in range(N):
            psend[ar, j] = part[ROWS * (j // 4):ROWS * (j // 4) + ROWS, COLS * (j % 4):COLS * (j % 4) + COLS].astype(jnp.bfloat16)

    def rs_copy(ar, d):
        t = peers[d]
        return pltpu.make_async_remote_copy(
            src_ref=psend.at[ar, t], dst_ref=rsb.at[ar, d],
            send_sem=ar_ss, recv_sem=rs_rs.at[ar],
            device_id=dev(t), device_id_type=pl.DeviceIdType.MESH)

    def ag_copy(ar, d):
        t = peers[d]
        return pltpu.make_async_remote_copy(
            src_ref=hb.at[ar + 1, me], dst_ref=hb.at[ar + 1, me],
            send_sem=ar_ss, recv_sem=ag_rs.at[ar],
            device_id=dev(t), device_id_type=pl.DeviceIdType.MESH)

    def reduce_all(ar, filler=None):
        for d in range(N - 1):
            rs_copy(ar, d).start()
        if filler is not None:
            filler()
        total = psend[ar, me].astype(jnp.float32)
        landed(rsb.at[ar], rs_rs.at[ar])
        for d in range(N - 1):
            total = total + rsb[ar, d].astype(jnp.float32)
        hb[ar + 1, me] = (hb[ar, me].astype(jnp.float32) + total).astype(jnp.bfloat16)
        for d in range(N - 1):
            ag_copy(ar, d).start()

    def gather_wait(ar):
        landed(rsb.at[ar], ag_rs.at[ar])

    out_refs = (outs1, outs2)

    def write_caches(l):
        def chunk(c, _):
            for i in range(8):
                out_refs[l][c * 8 + i] = recv[l, 2 * c + i // 4, :, i % 4].reshape(SEQ, LANES).T
            return 0
        lax.fori_loop(0, CH, chunk, 0)

    def turn(l, lo, hi):
        def quad(j, _):
            rows = weight_rows(j)
            landed(wg.at[l, pl.ds(0, SLOTS)], s_w.at[l, j])
            for w in (wg, wu):
                for k in range(6):
                    cols = pl.ds(TILE * k, TILE)
                    w[l, rows, cols] = w[l, rows, cols].T
            return 0
        lax.fori_loop(lo, hi, quad, 0)

    lane_w = lax.broadcasted_iota(jnp.int32, (B, LANES), 1) < HEAD

    def experts(l, ar):
        norm_into(ar, gm, l)

        def up(j):
            rows = weight_rows(j)
            g = u = None
            for k in range(6):
                cols = pl.ds(TILE * k, TILE)
                x = m_s[:, cols]
                dg, du = dot_nn(x, wg[l, rows, cols]), dot_nn(x, wu[l, rows, cols])
                g, u = (dg, du) if g is None else (g + dg, u + du)
            act[j] = g * jax.nn.sigmoid(g) * u

        logits = dot_nt(m_s[...], wr[l])
        up(0)
        up(1)
        chosen = mask_s[l][:, 0:40] > 0.5
        top = jnp.max(jnp.where(chosen, logits, -jnp.inf), axis=-1, keepdims=True)
        e = jnp.where(chosen, jnp.exp(jnp.where(chosen, logits - top, 0.0)), 0.0)
        gate = e / jnp.sum(e, axis=-1, keepdims=True)
        for j in range(QUADS):
            for i in range(2):
                k = 4 * j + 2 * i
                g0 = jnp.broadcast_to(gate[:, k:k + 1], (B, LANES))
                g1 = jnp.broadcast_to(gate[:, k + 1:k + 2], (B, LANES))
                gx[j, :, pl.ds(LANES * i, LANES)] = jnp.where(left, g0, g1)
        for j in range(2, QUADS):
            up(j)
        landed(wd.at[l], s_d.at[l])
        for j in range(QUADS):
            acts[:, pl.ds(TILE * j, TILE)] = (gx[j] * act[j]).astype(jnp.bfloat16)
        for half in range(2):
            part = dot_nn(acts[...], wd[l, :, pl.ds(WIDE * half, WIDE)])
            for j in range(N):
                if (j % 4) // 2 == half:
                    lo = COLS * (j % 2)
                    psend[ar, j] = part[ROWS * (j // 4):ROWS * (j // 4) + ROWS, lo:lo + COLS].astype(jnp.bfloat16)

    SC = jax.named_scope
    with SC("p_proj0"):
        project(0, 0)
    with SC("p_prep1"):
        for c in range(CH):
            prep(1, c)
        a2a_send(1, 0)
    with SC("p_turn0"):
        turn(0, 0, 10)
    with SC("p_att0"):
        attend(0)
    with SC("p_aout0"):
        attn_out(0, 0)

    def fill_rs0():
        a2a_send(1, 1)
        a2a_send(1, 2)
        write_caches(0)

    with SC("p_rs0"):
        reduce_all(0, fill_rs0)
    with SC("p_ag0"):
        a2a_send(1, 3)
        a2a_send(1, 4)
        turn(1, 0, 4)
        gather_wait(0)
    for p in range(5, TP):
        a2a_send(1, p)
    with SC("p_moe0"):
        experts(0, 1)
    with SC("p_rs1"):
        reduce_all(1, lambda: turn(1, 4, 6))
    with SC("p_ag1"):
        turn(1, 6, 8)
        gather_wait(1)
    with SC("p_proj1"):
        project(1, 2)
    with SC("p_att1"):
        attend(1)
    with SC("p_aout1"):
        attn_out(1, 2)
    with SC("p_rs2"):
        reduce_all(2, lambda: write_caches(1))
    with SC("p_ag2"):
        turn(1, 8, 10)
        gather_wait(2)
    with SC("p_moe1"):
        experts(1, 3)
    with SC("p_rs3"):
        reduce_all(3)
    with SC("p_ag3"):
        gather_wait(3)
    with SC("p_end"):
        for j in range(N):
            hid_o[pl.ds(ROWS * (j // 4), ROWS), pl.ds(COLS * (j % 4), COLS)] = hb[4, j]
        landed(send.at[:, :, pl.ds(0, N - 1)], a2a_ss)
        landed(rsb, ar_ss)
        landed(rsb, ar_ss)


def tail_kernel(hid, kv1, kv2, hid_o, k1_o, v1_o, k2_o, v2_o, sem):
    copies = [
        (kv1.at[:, pl.ds(0, HEAD)], k1_o), (kv1.at[:, pl.ds(HEAD, HEAD)], v1_o),
        (kv2.at[:, pl.ds(0, HEAD)], k2_o), (kv2.at[:, pl.ds(HEAD, HEAD)], v2_o),
        (hid, hid_o),
    ]
    cps = [pltpu.make_async_copy(src, dst, sem.at[i]) for i, (src, dst) in enumerate(copies)]
    for cp in cps:
        cp.start()
    for cp in cps:
        cp.wait()


def solution(mesh):
    seq_spec = P('dp', 'tp', None, None)
    head_spec = P('dp', None, 'tp', None)
    col_spec = P(None, None, 'tp')
    ff_spec = P(None, None, None, 'tp')
    cos, sin = rope_tables()

    def local_step(hidden, lengths, choice, keys_one, vals_one, keys_two, vals_two, g_attn, w_q, w_k, w_v, w_o, g_mlp, w_router, w_gate, w_up, w_down):
        bf, f32 = jnp.bfloat16, jnp.float32
        any_spec = pl.BlockSpec(memory_space=pl.ANY)
        vmem_spec = pl.BlockSpec(memory_space=pltpu.VMEM)
        dma = pltpu.SemaphoreType.DMA
        vm = pltpu.VMEM
        operands = (
            lengths, hidden, jnp.swapaxes(choice, 1, 2),
            keys_one.reshape(SLOTS, 8, HEAD), vals_one.reshape(SLOTS, 8, HEAD), keys_two.reshape(SLOTS, 8, HEAD), vals_two.reshape(SLOTS, 8, HEAD),
            g_attn, jnp.swapaxes(w_q, 1, 2), jnp.swapaxes(w_k, 1, 2), jnp.swapaxes(w_v, 1, 2), w_o, g_mlp, jnp.swapaxes(w_router, 1, 2),
            jnp.swapaxes(w_gate, 2, 3).reshape(2, 2560, D), jnp.swapaxes(w_up, 2, 3).reshape(2, 2560, D), w_down.reshape(2, 2560, D),
            jnp.asarray(cos), jnp.asarray(sin),
        )
        hid, kv1, kv2 = pl.pallas_call(
            kernel,
            name='decode_two',
            out_shape=[vm((B, D), bf), vm((B, LANES, LANES), bf), vm((B, LANES, LANES), bf)],
            in_specs=[pl.BlockSpec(memory_space=pltpu.SMEM)] + [any_spec] * 18,
            out_specs=[vmem_spec] * 3,
            scratch_shapes=[
                vm((2, 2560, D), bf), vm((2, 2560, D), bf), vm((2, 2560, D), bf),
                vm((2, COLS, D), bf), vm((2, 192, D), bf), vm((2, 40, D), bf),
                vm((2, SLOTS, 8, HEAD), bf), vm((2, SLOTS, 8, HEAD), bf), vm((1024, LANES), f32),
                vm((2, TP, 8, 4, ROWS, LANES), bf), vm((2, TP, 8, 4, ROWS, LANES), bf),
                vm((5, 8, ROWS, COLS), bf), vm((4, 8, ROWS, COLS), bf), vm((4, 7, ROWS, COLS), bf),
                vm((B, D), bf), vm((TILE, LANES), f32), vm((8, LANES), f32), vm((TILE, LANES), f32), vm((B, LANES), f32),
                vm((LANES, LANES), f32), vm((LANES, LANES), f32), vm((B, LANES), f32), vm((B, LANES), f32),
                vm((2, 8, B), jnp.int32), vm((2, D), bf), vm((2, D), bf),
                vm((2, B, LANES), f32), vm((QUADS, B, TILE), f32), vm((QUADS, B, TILE), f32), vm((B, 2560), bf),
                dma((2, CH)), dma((2, QUADS)), dma((2,)), dma, dma, dma((2, TP)), dma, dma((4,)), dma((4,)),
            ],
            compiler_params=pltpu.CompilerParams(collective_id=0, has_side_effects=True, vmem_limit_bytes=63500000),
        )(*operands)
        hid_out, *caches = pl.pallas_call(
            tail_kernel,
            name='write_out',
            out_shape=[jax.ShapeDtypeStruct((B, D), bf)] + [jax.ShapeDtypeStruct((B, HEAD, LANES), bf)] * 4,
            in_specs=[vmem_spec] * 3,
            out_specs=[any_spec] * 5,
            scratch_shapes=[dma((5,))],
            compiler_params=pltpu.CompilerParams(vmem_limit_bytes=4 << 20),
        )(hid, kv1, kv2)
        return (hid_out, *[jnp.swapaxes(kv, 1, 2)[:, :, None, :] for kv in caches])

    return jax.shard_map(local_step, mesh=mesh, in_specs=(P('dp', None), P('dp'), P(None, 'dp', None), seq_spec, seq_spec, seq_spec, seq_spec, P(), col_spec, col_spec, col_spec, P(None, 'tp', None), P(), P(), ff_spec, ff_spec, P(None, None, 'tp', None)), out_specs=(P('dp', None), head_spec, head_spec, head_spec, head_spec), check_vma=False)
```

```python
import jax
import jax.numpy as jnp
import numpy as np
from jax import lax
from jax.experimental import pallas as pl
from jax.experimental.pallas import tpu as pltpu
from jax.sharding import PartitionSpec as P

EPS = 1e-5
THETA = 1000000.0
N = 8
B = 32
D = 1536
SEQ = 128
LANES, HEAD, ROWS, COLS, TILE, SLOTS, WIDE = 128, 64, 16, 384, 256, 512, 768
CH = 4
TP = 8
QUADS = 10
NT = (((1,), (1,)), ((), ()))
PEERS = ((1, 1, 0), (1, 1, 1), (1, 0, 1), (0, 1, 0), (1, 0, 0), (0, 1, 1), (0, 0, 1))


def rope_tables():
    half = 32
    inv = np.power(np.float32(THETA), (-2.0 * np.arange(half, dtype=np.float32) / HEAD).astype(np.float32)).astype(np.float32)
    angle = (np.arange(SEQ, dtype=np.float32)[:, None] * inv[None, :]).astype(np.float32).astype(np.float64)
    cos = np.tile(np.cos(angle), (1, 4)).astype(np.float32)
    sin = np.tile(np.sin(angle), (1, 4)).astype(np.float32)
    return cos, sin


def dot_nt(a, b):
    return lax.dot_general(a, b, NT, preferred_element_type=jnp.float32)


def dot_nn(a, b):
    return jnp.dot(a, b, preferred_element_type=jnp.float32)


def kernel(len_h, hid_h, choice_h, k1_h, v1_h, k2_h, v2_h, ga_h, wq_h, wk_h, wv_h, wo_h, gm_h, wr_h, wg_h, wu_h, wd_h, cos_h, sin_h,
           hid_o, outs1, outs2,
           len_s, wg, wu, wd, wqkv, wo, wr, xk, xv, stage, send, recv, hb, psend, rsb, m_s, qs, sc, os_, kvn, cos_t, sin_t, cos_b, sin_b, choice_v, ga, gm, mask_s, gx, act, acts,
           s_in, s_w, s_d, s_small, a2a_ss, a2a_rs, ar_ss, rs_rs, ag_rs):
    me = lax.axis_index('tp')
    my, mx, mc = me // 4, (me // 2) % 2, me % 2
    peers = []
    for dy, dx, dc in PEERS:
        peers.append(((my + dy) % 2) * 4 + ((mx + dx) % 2) * 2 + (mc + dc) % 2)

    def dev(t):
        return {'tp': t}

    def landed(like, sem):
        pltpu.make_async_copy(like, like, sem).wait()

    caches = ((k1_h, v1_h), (k2_h, v2_h))
    cache_cp = {}
    for l in range(2):
        for c in range(CH):
            for i, buf in enumerate((xk, xv)):
                rows = pl.ds(c * LANES, LANES)
                cp = pltpu.make_async_copy(caches[l][i].at[rows], buf.at[l, rows], s_in.at[c if l == 0 else CH])
                cache_cp[l, c, i] = cp

    for c in range(CH):
        cache_cp[0, c, 0].start()
        cache_cp[0, c, 1].start()

    barrier = pltpu.get_barrier_semaphore()
    for t in peers:
        pl.semaphore_signal(barrier, inc=1, device_id=dev(t), device_id_type=pl.DeviceIdType.MESH)

    small = [
        (len_h, len_s), (cos_h, cos_t), (sin_h, sin_t), (choice_h, choice_v), (ga_h, ga), (gm_h, gm), (wr_h, wr), (wo_h, wo),
    ]
    for l in range(2):
        small.append((wq_h.at[l, pl.ds(0, LANES)], wqkv.at[l, pl.ds(0, LANES)]))
        small.append((wk_h.at[l], wqkv.at[l, pl.ds(LANES, HEAD)]))
        small.append((wq_h.at[l, pl.ds(LANES, HEAD)], wqkv.at[l, pl.ds(192, HEAD)]))
        small.append((wv_h.at[l], wqkv.at[l, pl.ds(320, HEAD)]))
    for j in range(N):
        small.append((hid_h.at[pl.ds(ROWS * (j // 4), ROWS), pl.ds(COLS * (j % 4), COLS)], hb.at[0, j]))
    small_cp = [pltpu.make_async_copy(src, dst, s_small) for src, dst in small]

    def weight_rows(j):
        return pl.ds(pl.multiple_of(j * TILE, TILE), TILE)

    def start_rest():
        for cp in small_cp:
            cp.start()
        for c in range(CH):
            cache_cp[1, c, 0].start()
            cache_cp[1, c, 1].start()
        for l in range(2):
            def start_gate_up(j, _, l=l):
                rows = weight_rows(j)
                pltpu.make_async_copy(wg_h.at[l, rows], wg.at[l, rows], s_w.at[j if l == 0 else QUADS]).start()
                pltpu.make_async_copy(wu_h.at[l, rows], wu.at[l, rows], s_w.at[j if l == 0 else QUADS]).start()
                return 0
            lax.fori_loop(0, QUADS, start_gate_up, 0)
            def start_down(j, _, l=l):
                rows = weight_rows(j)
                pltpu.make_async_copy(wd_h.at[l, rows], wd.at[l, rows], s_d.at[l]).start()
                return 0
            lax.fori_loop(0, QUADS, start_down, 0)

    def prep(l, c):
        if l == 0:
            landed(xk.at[l, pl.ds(0, TILE)], s_in.at[c])
        for i in range(2):
            rows = pl.ds(c * LANES + i * HEAD, HEAD)
            kk = xk[l, rows].astype(jnp.float32)
            vv = xv[l, rows].astype(jnp.float32)
            stage[pl.ds(i * SLOTS, SLOTS), :] = jnp.concatenate([kk, vv], axis=-1).reshape(SLOTS, LANES)
        for h in range(N):
            rows = stage[pl.ds(h, LANES, stride=8), :].astype(jnp.bfloat16).reshape(2, 4, ROWS, LANES)
            send[l, 2 * c, h] = rows[0]
            send[l, 2 * c + 1, h] = rows[1]

    def a2a_copy(l, p, d):
        t = peers[d]
        return pltpu.make_async_remote_copy(
            src_ref=send.at[l, p, t], dst_ref=recv.at[l, p, me],
            send_sem=a2a_ss, recv_sem=a2a_rs.at[p // 2 if l == 0 else CH],
            device_id=dev(t), device_id_type=pl.DeviceIdType.MESH)

    def a2a_send(l, p):
        for d in range(N - 1):
            a2a_copy(l, p, d).start()
        if l == 0:
            recv[l, p, me] = send[l, p, me]

    with jax.named_scope('p_prep0'):
        prep(0, 0)
    with jax.named_scope('p_bar'):
        pl.semaphore_wait(barrier, N - 1)
    with jax.named_scope('p_send0'):
        a2a_send(0, 0)
        a2a_send(0, 1)
        for c in range(1, CH):
            prep(0, c)
            a2a_send(0, 2 * c)
            a2a_send(0, 2 * c + 1)
    with jax.named_scope('p_rest'):
        start_rest()

    for cp in small_cp:
        cp.wait()
    for l in range(2):
        wqkv[l, pl.ds(TILE, HEAD), :] = jnp.zeros((HEAD, D), jnp.bfloat16)
    qs[...] = jnp.zeros_like(qs)

    def rope_rows(b, _):
        pos = len_s[b]
        cos_b[pl.ds(b, 1), :] = cos_t[pl.ds(pos, 1), :]
        sin_b[pl.ds(b, 1), :] = sin_t[pl.ds(pos, 1), :]
        return 0
    lax.fori_loop(0, B, rope_rows, 0)

    for l in range(2):
        ids = lax.broadcasted_iota(jnp.int32, (LANES, B), 0)
        picked = jnp.zeros((LANES, B), jnp.float32)
        for k in range(8):
            picked = jnp.where(ids == choice_v[l, pl.ds(k, 1), :], 1.0, picked)
        mask_s[l] = picked.T

    lane = lax.broadcasted_iota(jnp.int32, (B, LANES), 1)
    left = lane < HEAD
    lower = (lane % HEAD) < 32

    def norm_into(src, gain_ref, l):
        for hf in range(2):
            xs = [hb[src, 4 * hf + c].astype(jnp.float32) for c in range(4)]
            sq = xs[0] * xs[0]
            for x in xs[1:]:
                sq = sq + x * x
            scale = lax.rsqrt(jnp.sum(sq, axis=-1, keepdims=True) * (1.0 / D) + EPS)
            for c in range(4):
                g = gain_ref[pl.ds(l, 1), pl.ds(COLS * c, COLS)].astype(jnp.float32)
                m_s[pl.ds(ROWS * hf, ROWS), pl.ds(COLS * c, COLS)] = (xs[c] * scale * g).astype(jnp.bfloat16)

    def rope(x):
        rot = jnp.where(lower, -pltpu.roll(x, 96, 1), pltpu.roll(x, 32, 1))
        return x * cos_b[...] + rot * sin_b[...]

    def rounded(x):
        return x.astype(jnp.bfloat16).astype(jnp.float32)

    def project(l, src):
        norm_into(src, ga, l)
        if l == 0:
            qkv = dot_nt(m_s[...], wqkv[l])
        else:
            qkv = None
            for k in range(6):
                tile = jnp.concatenate([jnp.concatenate([
                    wqkv[l, pl.ds(LANES * a, LANES), pl.ds(LANES * i, LANES)] for i in (2 * k, 2 * k + 1)], axis=0) for a in range(3)], axis=1)
                part = dot_nn(m_s[:, pl.ds(TILE * k, TILE)], tile)
                qkv = part if qkv is None else qkv + part
        qa = rounded(rope(qkv[:, 0:LANES]))
        kq = rounded(rope(qkv[:, LANES:TILE]))
        zero = jnp.zeros_like(qa)
        qs[pl.ds(0, B, stride=8), :] = jnp.where(left, qa, zero)
        qs[pl.ds(1, B, stride=8), :] = jnp.where(left, pltpu.roll(qa, HEAD, 1), zero)
        qs[pl.ds(2, B, stride=8), :] = jnp.where(left, pltpu.roll(kq, HEAD, 1), zero)
        kvn[...] = jnp.where(left, kq, rounded(qkv[:, TILE:COLS]))

    row_ids = lax.broadcasted_iota(jnp.int32, (SEQ, LANES), 0)
    lane8 = lax.broadcasted_iota(jnp.int32, (8, LANES), 1)

    def attend(l):
        def chunk(c, _):
            landed(recv.at[l, pl.ds(0, 2), pl.ds(0, N - 1)], a2a_rs.at[c])
            tiles, scores = [], []
            for i in range(8):
                b = c * 8 + i
                pos = len_s[b]
                tile = recv[l, 2 * c + i // 4, :, i % 4].reshape(SEQ, LANES).astype(jnp.float32)
                tile = jnp.where(row_ids == pos, kvn[pl.ds(b, 1), :], tile).astype(jnp.bfloat16)
                recv[l, 2 * c + i // 4, :, i % 4] = tile.reshape(8, ROWS, LANES)
                q = qs[pl.ds(pl.multiple_of(b * 8, 8), 8), :].astype(jnp.bfloat16)
                scores.append(jnp.where(lane8 <= pos, dot_nt(q, tile) * 0.125, -1e30))
                tiles.append(tile)
            s = jnp.concatenate(scores, axis=0)
            e = jnp.exp(s - jnp.max(s, axis=-1, keepdims=True))
            p = e / jnp.sum(e, axis=-1, keepdims=True)
            for i in range(8):
                b = c * 8 + i
                o = dot_nn(p[8 * i:8 * i + 8].astype(jnp.bfloat16), tiles[i])
                os_[pl.ds(pl.multiple_of(b * 8, 8), 8), :] = o
            return 0
        lax.fori_loop(0, CH, chunk, 0)

    def attend_all(l):
        landed(recv.at[l, :, pl.ds(0, N - 1)], a2a_rs.at[CH])
        for b in range(B):
            pos = len_s[b]
            spot = recv.at[l, b // 4, :, b % 4]
            tile = spot[...].reshape(SEQ, LANES).astype(jnp.float32)
            tile = jnp.where(row_ids == pos, kvn[pl.ds(b, 1), :], tile).astype(jnp.bfloat16)
            spot[...] = tile.reshape(8, ROWS, LANES)
            q = qs[pl.ds(b * 8, 8), :].astype(jnp.bfloat16)
            sc[pl.ds(b * 8, 8), :] = jnp.where(lane8 <= pos, dot_nt(q, tile) * 0.125, -1e30)
        s = sc[...]
        e = jnp.exp(s - jnp.max(s, axis=-1, keepdims=True))
        sc[...] = e / jnp.sum(e, axis=-1, keepdims=True)
        for b in range(B):
            p = sc[pl.ds(b * 8, 8), :].astype(jnp.bfloat16)
            os_[pl.ds(b * 8, 8), :] = dot_nn(p, recv[l, b // 4, :, b % 4].reshape(SEQ, LANES))

    def attn_out(l, ar):
        o0 = os_[pl.ds(0, B, stride=8), :]
        o1 = os_[pl.ds(1, B, stride=8), :]
        o2 = os_[pl.ds(2, B, stride=8), :]
        oa = jnp.where(left, pltpu.roll(o0, HEAD, 1), o1).astype(jnp.bfloat16)
        ob = pltpu.roll(o2, HEAD, 1)[:, 0:HEAD].astype(jnp.bfloat16)
        send_halves(ar, lambda cols: dot_nn(oa, wo[l, pl.ds(0, LANES), cols]) + dot_nn(ob, wo[l, pl.ds(LANES, HEAD), cols]))

    def send_halves(ar, columns):
        for dx in (1, 0):
            xs = (mx + dx) % 2
            part = columns(pl.ds(pl.multiple_of(WIDE * xs, LANES), WIDE))
            for hy in range(2):
                for c in range(2):
                    psend[ar, 4 * hy + 2 * xs + c] = part[ROWS * hy:ROWS * hy + ROWS, COLS * c:COLS * c + COLS].astype(jnp.bfloat16)
            for d in range(N - 1):
                if PEERS[d][1] == dx:
                    rs_copy(ar, d).start()

    def rs_copy(ar, d):
        t = peers[d]
        return pltpu.make_async_remote_copy(
            src_ref=psend.at[ar, t], dst_ref=rsb.at[ar, d],
            send_sem=ar_ss, recv_sem=rs_rs.at[ar],
            device_id=dev(t), device_id_type=pl.DeviceIdType.MESH)

    def ag_copy(ar, d):
        t = peers[d]
        return pltpu.make_async_remote_copy(
            src_ref=hb.at[ar + 1, me], dst_ref=hb.at[ar + 1, me],
            send_sem=ar_ss, recv_sem=ag_rs.at[ar],
            device_id=dev(t), device_id_type=pl.DeviceIdType.MESH)

    def reduce_all(ar, filler=None):
        if filler is not None:
            filler()
        total = psend[ar, me].astype(jnp.float32)
        landed(rsb.at[ar], rs_rs.at[ar])
        for d in range(N - 1):
            total = total + rsb[ar, d].astype(jnp.float32)
        hb[ar + 1, me] = (hb[ar, me].astype(jnp.float32) + total).astype(jnp.bfloat16)
        for d in range(N - 1):
            ag_copy(ar, d).start()

    def gather_wait(ar):
        landed(rsb.at[ar], ag_rs.at[ar])

    out_refs = (outs1, outs2)

    def write_caches(l):
        def chunk(c, _):
            for i in range(8):
                out_refs[l][c * 8 + i] = recv[l, 2 * c + i // 4, :, i % 4].reshape(SEQ, LANES).T
            return 0
        lax.fori_loop(0, CH, chunk, 0)

    def turn(l, lo, hi):
        def quad(j, _):
            rows = weight_rows(j)
            if l == 0:
                landed(wg.at[l, pl.ds(0, SLOTS)], s_w.at[j])
            for w in (wg, wu):
                for k in range(6):
                    cols = pl.ds(TILE * k, TILE)
                    w[l, rows, cols] = w[l, rows, cols].T
            return 0
        lax.fori_loop(lo, hi, quad, 0)

    def turn_projection(l):
        for a in range(3):
            for i in range(12):
                spot = wqkv.at[l, pl.ds(LANES * a, LANES), pl.ds(LANES * i, LANES)]
                spot[...] = spot[...].T

    lane_w = lax.broadcasted_iota(jnp.int32, (B, LANES), 1) < HEAD

    def experts(l, ar, pieces=()):
        norm_into(ar, gm, l)

        def up(j):
            rows = weight_rows(j)
            g = u = None
            for k in range(6):
                cols = pl.ds(TILE * k, TILE)
                x = m_s[:, cols]
                dg, du = dot_nn(x, wg[l, rows, cols]), dot_nn(x, wu[l, rows, cols])
                g, u = (dg, du) if g is None else (g + dg, u + du)
            act[j] = g * jax.nn.sigmoid(g) * u

        logits = dot_nt(m_s[...], wr[l])
        for p in pieces:
            a2a_send(1, p)
        up(0)
        up(1)
        chosen = mask_s[l][:, 0:40] > 0.5
        top = jnp.max(jnp.where(chosen, logits, -jnp.inf), axis=-1, keepdims=True)
        e = jnp.where(chosen, jnp.exp(jnp.where(chosen, logits - top, 0.0)), 0.0)
        gate = e / jnp.sum(e, axis=-1, keepdims=True)
        for j in range(QUADS):
            for i in range(2):
                k = 4 * j + 2 * i
                g0 = jnp.broadcast_to(gate[:, k:k + 1], (B, LANES))
                g1 = jnp.broadcast_to(gate[:, k + 1:k + 2], (B, LANES))
                gx[j, :, pl.ds(LANES * i, LANES)] = jnp.where(left, g0, g1)
        for j in range(2, QUADS):
            up(j)
        landed(wd.at[l], s_d.at[l])
        for j in range(QUADS):
            acts[:, pl.ds(TILE * j, TILE)] = (gx[j] * act[j]).astype(jnp.bfloat16)
        send_halves(ar, lambda cols: dot_nn(acts[...], wd[l, :, cols]))

    SC = jax.named_scope
    with SC("p_proj0"):
        project(0, 0)
    with SC("p_prep1"):
        landed(xk, s_in.at[CH])
        for c in range(CH):
            prep(1, c)
        recv[1, :, me] = send[1, :, me]
    with SC("p_turn0"):
        turn_projection(1)
        turn(0, 0, 10)
    with SC("p_att0"):
        attend(0)
    with SC("p_aout0"):
        attn_out(0, 0)

    def fill_rs0():
        a2a_send(1, 0)
        a2a_send(1, 1)
        write_caches(0)

    with SC("p_rs0"):
        reduce_all(0, fill_rs0)
    with SC("p_ag0"):
        a2a_send(1, 2)
        a2a_send(1, 3)
        landed(wg, s_w.at[QUADS])
        turn(1, 0, 4)
        gather_wait(0)
    for p in range(4, 7):
        a2a_send(1, p)
    with SC("p_moe0"):
        experts(0, 1)
    with SC("p_rs1"):
        reduce_all(1, lambda: turn(1, 4, 6))
    with SC("p_ag1"):
        a2a_send(1, 7)
        turn(1, 6, 8)
        gather_wait(1)
    with SC("p_proj1"):
        project(1, 2)
    with SC("p_att1"):
        attend_all(1)
    with SC("p_aout1"):
        attn_out(1, 2)
    with SC("p_rs2"):
        reduce_all(2, lambda: write_caches(1))
    with SC("p_ag2"):
        turn(1, 8, 10)
        gather_wait(2)
    with SC("p_moe1"):
        experts(1, 3)
    with SC("p_rs3"):
        reduce_all(3)
    with SC("p_ag3"):
        gather_wait(3)
    with SC("p_end"):
        for j in range(N):
            hid_o[pl.ds(ROWS * (j // 4), ROWS), pl.ds(COLS * (j % 4), COLS)] = hb[4, j]
        landed(send.at[:, :, pl.ds(0, N - 1)], a2a_ss)
        landed(rsb, ar_ss)
        landed(rsb, ar_ss)


def tail_kernel(hid, kv1, kv2, hid_o, k1_o, v1_o, k2_o, v2_o, sem):
    copies = [
        (kv1.at[:, pl.ds(0, HEAD)], k1_o), (kv1.at[:, pl.ds(HEAD, HEAD)], v1_o),
        (kv2.at[:, pl.ds(0, HEAD)], k2_o), (kv2.at[:, pl.ds(HEAD, HEAD)], v2_o),
        (hid, hid_o),
    ]
    cps = [pltpu.make_async_copy(src, dst, sem.at[i]) for i, (src, dst) in enumerate(copies)]
    for cp in cps:
        cp.start()
    for cp in cps:
        cp.wait()


def solution(mesh):
    seq_spec = P('dp', 'tp', None, None)
    head_spec = P('dp', None, 'tp', None)
    col_spec = P(None, None, 'tp')
    ff_spec = P(None, None, None, 'tp')
    cos, sin = rope_tables()

    def local_step(hidden, lengths, choice, keys_one, vals_one, keys_two, vals_two, g_attn, w_q, w_k, w_v, w_o, g_mlp, w_router, w_gate, w_up, w_down):
        bf, f32 = jnp.bfloat16, jnp.float32
        any_spec = pl.BlockSpec(memory_space=pl.ANY)
        vmem_spec = pl.BlockSpec(memory_space=pltpu.VMEM)
        dma = pltpu.SemaphoreType.DMA
        vm = pltpu.VMEM
        operands = (
            lengths, hidden, jnp.swapaxes(choice, 1, 2),
            keys_one.reshape(SLOTS, 8, HEAD), vals_one.reshape(SLOTS, 8, HEAD), keys_two.reshape(SLOTS, 8, HEAD), vals_two.reshape(SLOTS, 8, HEAD),
            g_attn, jnp.swapaxes(w_q, 1, 2), jnp.swapaxes(w_k, 1, 2), jnp.swapaxes(w_v, 1, 2), w_o, g_mlp, jnp.swapaxes(w_router, 1, 2),
            jnp.swapaxes(w_gate, 2, 3).reshape(2, 2560, D), jnp.swapaxes(w_up, 2, 3).reshape(2, 2560, D), w_down.reshape(2, 2560, D),
            jnp.asarray(cos), jnp.asarray(sin),
        )
        hid, kv1, kv2 = pl.pallas_call(
            kernel,
            name='decode_two',
            out_shape=[vm((B, D), bf), vm((B, LANES, LANES), bf), vm((B, LANES, LANES), bf)],
            in_specs=[any_spec] * 19,
            out_specs=[vmem_spec] * 3,
            scratch_shapes=[
                pltpu.SMEM((B,), jnp.int32),
                vm((2, 2560, D), bf), vm((2, 2560, D), bf), vm((2, 2560, D), bf),
                vm((2, COLS, D), bf), vm((2, 192, D), bf), vm((2, 40, D), bf),
                vm((2, SLOTS, 8, HEAD), bf), vm((2, SLOTS, 8, HEAD), bf), vm((1024, LANES), f32),
                vm((2, TP, 8, 4, ROWS, LANES), bf), vm((2, TP, 8, 4, ROWS, LANES), bf),
                vm((5, 8, ROWS, COLS), bf), vm((4, 8, ROWS, COLS), bf), vm((4, 7, ROWS, COLS), bf),
                vm((B, D), bf), vm((TILE, LANES), f32), vm((TILE, LANES), f32), vm((TILE, LANES), f32), vm((B, LANES), f32),
                vm((LANES, LANES), f32), vm((LANES, LANES), f32), vm((B, LANES), f32), vm((B, LANES), f32),
                vm((2, 8, B), jnp.int32), vm((2, D), bf), vm((2, D), bf),
                vm((2, B, LANES), f32), vm((QUADS, B, TILE), f32), vm((QUADS, B, TILE), f32), vm((B, 2560), bf),
                dma((CH + 1,)), dma((QUADS + 1,)), dma((2,)), dma, dma, dma((CH + 1,)), dma, dma((4,)), dma((4,)),
            ],
            compiler_params=pltpu.CompilerParams(collective_id=0, has_side_effects=True, vmem_limit_bytes=63500000),
        )(*operands)
        hid_out, *caches = pl.pallas_call(
            tail_kernel,
            name='write_out',
            out_shape=[jax.ShapeDtypeStruct((B, D), bf)] + [jax.ShapeDtypeStruct((B, HEAD, LANES), bf)] * 4,
            in_specs=[vmem_spec] * 3,
            out_specs=[any_spec] * 5,
            scratch_shapes=[dma((5,))],
            compiler_params=pltpu.CompilerParams(vmem_limit_bytes=4 << 20),
        )(hid, kv1, kv2)
        return (hid_out, *[jnp.swapaxes(kv, 1, 2)[:, :, None, :] for kv in caches])

    return jax.shard_map(local_step, mesh=mesh, in_specs=(P('dp', None), P('dp'), P(None, 'dp', None), seq_spec, seq_spec, seq_spec, seq_spec, P(), col_spec, col_spec, col_spec, P(None, 'tp', None), P(), P(), ff_spec, ff_spec, P(None, None, 'tp', None)), out_specs=(P('dp', None), head_spec, head_spec, head_spec, head_spec), check_vma=False)
```

```python
import jax
import jax.numpy as jnp
import numpy as np
from jax import lax
from jax.experimental import pallas as pl
from jax.experimental.pallas import tpu as pltpu
from jax.sharding import PartitionSpec as P

EPS = 1e-5
THETA = 1000000.0
N = 8
B = 32
D = 1536
SEQ = 128
LANES, HEAD, ROWS, COLS, TILE, SLOTS, WIDE = 128, 64, 16, 384, 256, 512, 768
CH = 4
TP = 8
QUADS = 10
NT = (((1,), (1,)), ((), ()))
PEERS = ((1, 1, 0), (1, 1, 1), (1, 0, 1), (0, 1, 0), (1, 0, 0), (0, 1, 1), (0, 0, 1))


def rope_tables():
    half = 32
    inv = np.power(np.float32(THETA), (-2.0 * np.arange(half, dtype=np.float32) / HEAD).astype(np.float32)).astype(np.float32)
    angle = (np.arange(SEQ, dtype=np.float32)[:, None] * inv[None, :]).astype(np.float32).astype(np.float64)
    cos = np.tile(np.cos(angle), (1, 4)).astype(np.float32)
    sin = np.tile(np.sin(angle), (1, 4)).astype(np.float32)
    return cos, sin


def dot_nt(a, b):
    return lax.dot_general(a, b, NT, preferred_element_type=jnp.float32)


def dot_nn(a, b):
    return jnp.dot(a, b, preferred_element_type=jnp.float32)


def kernel(len_h, hid_h, choice_h, k1_h, v1_h, k2_h, v2_h, ga_h, wq_h, wk_h, wv_h, wo_h, gm_h, wr_h, wg_h, wu_h, wd_h, cos_h, sin_h,
           hid_o, outs1, outs2,
           len_s, wg, wu, wd, wqkv, wo, wr, xk, xv, stage, send, recv, hb, psend, rsb, m_s, qs, os_, kvn, cos_t, sin_t, cos_b, sin_b, choice_v, ga, gm, mask_s, gx, act, acts,
           s_in, s_w, s_d, s_small, a2a_ss, a2a_rs, ar_ss, rs_rs, ag_rs):
    me = lax.axis_index('tp')
    my, mx, mc = me // 4, (me // 2) % 2, me % 2
    peers = []
    for dy, dx, dc in PEERS:
        peers.append(((my + dy) % 2) * 4 + ((mx + dx) % 2) * 2 + (mc + dc) % 2)

    def dev(t):
        return {'tp': t}

    def landed(like, sem):
        pltpu.make_async_copy(like, like, sem).wait()

    caches = ((k1_h, v1_h), (k2_h, v2_h))
    cache_cp = {}
    for l in range(2):
        for c in range(CH):
            for i, buf in enumerate((xk, xv)):
                rows = pl.ds(c * LANES, LANES)
                cp = pltpu.make_async_copy(caches[l][i].at[rows], buf.at[l, rows], s_in.at[c if l == 0 else CH])
                cache_cp[l, c, i] = cp

    for c in range(CH):
        cache_cp[0, c, 0].start()
        cache_cp[0, c, 1].start()

    barrier = pltpu.get_barrier_semaphore()
    for t in peers:
        pl.semaphore_signal(barrier, inc=1, device_id=dev(t), device_id_type=pl.DeviceIdType.MESH)

    small = [
        (len_h, len_s), (cos_h, cos_t), (sin_h, sin_t), (choice_h, choice_v), (ga_h, ga), (gm_h, gm), (wr_h, wr), (wo_h, wo),
    ]
    for l in range(2):
        small.append((wq_h.at[l, pl.ds(0, LANES)], wqkv.at[l, pl.ds(0, LANES)]))
        small.append((wk_h.at[l], wqkv.at[l, pl.ds(LANES, HEAD)]))
        small.append((wq_h.at[l, pl.ds(LANES, HEAD)], wqkv.at[l, pl.ds(192, HEAD)]))
        small.append((wv_h.at[l], wqkv.at[l, pl.ds(320, HEAD)]))
    for j in range(N):
        small.append((hid_h.at[pl.ds(ROWS * (j // 4), ROWS), pl.ds(COLS * (j % 4), COLS)], hb.at[0, j]))
    small_cp = [pltpu.make_async_copy(src, dst, s_small) for src, dst in small]

    def weight_rows(j):
        return pl.ds(pl.multiple_of(j * TILE, TILE), TILE)

    def start_rest():
        for cp in small_cp:
            cp.start()
        for c in range(CH):
            cache_cp[1, c, 0].start()
            cache_cp[1, c, 1].start()
        for l in range(2):
            def start_gate_up(j, _, l=l):
                rows = weight_rows(j)
                pltpu.make_async_copy(wg_h.at[l, rows], wg.at[l, rows], s_w.at[l]).start()
                pltpu.make_async_copy(wu_h.at[l, rows], wu.at[l, rows], s_w.at[l]).start()
                return 0
            lax.fori_loop(0, QUADS, start_gate_up, 0)
            def start_down(j, _, l=l):
                rows = weight_rows(j)
                pltpu.make_async_copy(wd_h.at[l, rows], wd.at[l, rows], s_d.at[l]).start()
                return 0
            lax.fori_loop(0, QUADS, start_down, 0)

    def prep(l, c):
        if l == 0:
            landed(xk.at[l, pl.ds(0, TILE)], s_in.at[c])
        for i in range(2):
            rows = pl.ds(c * LANES + i * HEAD, HEAD)
            kk = xk[l, rows].astype(jnp.float32)
            vv = xv[l, rows].astype(jnp.float32)
            stage[pl.ds(i * SLOTS, SLOTS), :] = jnp.concatenate([kk, vv], axis=-1).reshape(SLOTS, LANES)
        for h in range(N):
            rows = stage[pl.ds(h, LANES, stride=8), :].astype(jnp.bfloat16).reshape(2, 4, ROWS, LANES)
            send[l, 2 * c, h] = rows[0]
            send[l, 2 * c + 1, h] = rows[1]

    def a2a_copy(l, p, d):
        t = peers[d]
        return pltpu.make_async_remote_copy(
            src_ref=send.at[l, p, t], dst_ref=recv.at[l, p, me],
            send_sem=a2a_ss, recv_sem=a2a_rs.at[p // 2 if l == 0 else CH],
            device_id=dev(t), device_id_type=pl.DeviceIdType.MESH)

    def a2a_send(l, p):
        for d in range(N - 1):
            a2a_copy(l, p, d).start()
        if l == 0:
            recv[l, p, me] = send[l, p, me]

    with jax.named_scope('p_prep0'):
        prep(0, 0)
    with jax.named_scope('p_bar'):
        pl.semaphore_wait(barrier, N - 1)
    with jax.named_scope('p_send0'):
        a2a_send(0, 0)
        a2a_send(0, 1)
        for c in range(1, CH):
            prep(0, c)
            a2a_send(0, 2 * c)
            a2a_send(0, 2 * c + 1)
    with jax.named_scope('p_rest'):
        start_rest()

    for cp in small_cp:
        cp.wait()
    for l in range(2):
        wqkv[l, pl.ds(TILE, HEAD), :] = jnp.zeros((HEAD, D), jnp.bfloat16)
    qs[...] = jnp.zeros_like(qs)

    def rope_rows(b, _):
        pos = len_s[b]
        cos_b[pl.ds(b, 1), :] = cos_t[pl.ds(pos, 1), :]
        sin_b[pl.ds(b, 1), :] = sin_t[pl.ds(pos, 1), :]
        return 0
    lax.fori_loop(0, B, rope_rows, 0)

    for l in range(2):
        ids = lax.broadcasted_iota(jnp.int32, (LANES, B), 0)
        picked = jnp.zeros((LANES, B), jnp.float32)
        for k in range(8):
            picked = jnp.where(ids == choice_v[l, pl.ds(k, 1), :], 1.0, picked)
        mask_s[l] = picked.T

    lane = lax.broadcasted_iota(jnp.int32, (B, LANES), 1)
    left = lane < HEAD
    lower = (lane % HEAD) < 32

    def norm_into(src, gain_ref, l):
        for hf in range(2):
            xs = [hb[src, 4 * hf + c].astype(jnp.float32) for c in range(4)]
            sq = xs[0] * xs[0]
            for x in xs[1:]:
                sq = sq + x * x
            scale = lax.rsqrt(jnp.sum(sq, axis=-1, keepdims=True) * (1.0 / D) + EPS)
            for c in range(4):
                g = gain_ref[pl.ds(l, 1), pl.ds(COLS * c, COLS)].astype(jnp.float32)
                m_s[pl.ds(ROWS * hf, ROWS), pl.ds(COLS * c, COLS)] = (xs[c] * scale * g).astype(jnp.bfloat16)

    def rope(x):
        rot = jnp.where(lower, -pltpu.roll(x, 96, 1), pltpu.roll(x, 32, 1))
        return x * cos_b[...] + rot * sin_b[...]

    def rounded(x):
        return x.astype(jnp.bfloat16).astype(jnp.float32)

    def project(l, src):
        norm_into(src, ga, l)
        if l == 0:
            qkv = dot_nt(m_s[...], wqkv[l])
        else:
            qkv = None
            for k in range(6):
                tile = jnp.concatenate([jnp.concatenate([
                    wqkv[l, pl.ds(LANES * a, LANES), pl.ds(LANES * i, LANES)] for i in (2 * k, 2 * k + 1)], axis=0) for a in range(3)], axis=1)
                part = dot_nn(m_s[:, pl.ds(TILE * k, TILE)], tile)
                qkv = part if qkv is None else qkv + part
        qa = rounded(rope(qkv[:, 0:LANES]))
        kq = rounded(rope(qkv[:, LANES:TILE]))
        zero = jnp.zeros_like(qa)
        qs[pl.ds(0, B, stride=8), :] = jnp.where(left, qa, zero)
        qs[pl.ds(1, B, stride=8), :] = jnp.where(left, pltpu.roll(qa, HEAD, 1), zero)
        qs[pl.ds(2, B, stride=8), :] = jnp.where(left, pltpu.roll(kq, HEAD, 1), zero)
        kvn[...] = jnp.where(left, kq, rounded(qkv[:, TILE:COLS]))

    row_ids = lax.broadcasted_iota(jnp.int32, (SEQ, LANES), 0)
    lane8 = lax.broadcasted_iota(jnp.int32, (8, LANES), 1)

    def attend(l):
        def chunk(c, _):
            landed(recv.at[l, pl.ds(0, 2), pl.ds(0, N - 1)], a2a_rs.at[c])
            tiles, scores = [], []
            for i in range(8):
                b = c * 8 + i
                pos = len_s[b]
                tile = recv[l, 2 * c + i // 4, :, i % 4].reshape(SEQ, LANES).astype(jnp.float32)
                tile = jnp.where(row_ids == pos, kvn[pl.ds(b, 1), :], tile).astype(jnp.bfloat16)
                recv[l, 2 * c + i // 4, :, i % 4] = tile.reshape(8, ROWS, LANES)
                q = qs[pl.ds(pl.multiple_of(b * 8, 8), 8), :].astype(jnp.bfloat16)
                scores.append(jnp.where(lane8 <= pos, dot_nt(q, tile) * 0.125, -1e30))
                tiles.append(tile)
            s = jnp.concatenate(scores, axis=0)
            e = jnp.exp(s - jnp.max(s, axis=-1, keepdims=True))
            p = e / jnp.sum(e, axis=-1, keepdims=True)
            for i in range(8):
                b = c * 8 + i
                o = dot_nn(p[8 * i:8 * i + 8].astype(jnp.bfloat16), tiles[i])
                os_[pl.ds(pl.multiple_of(b * 8, 8), 8), :] = o
            return 0
        lax.fori_loop(0, CH, chunk, 0)

    def attend_all(l):
        landed(recv.at[l, :, pl.ds(0, N - 1)], a2a_rs.at[CH])
        for b in range(B):
            pos = len_s[b]
            spot = recv.at[l, b // 4, :, b % 4]
            tile = spot[...].reshape(SEQ, LANES).astype(jnp.float32)
            tile = jnp.where(row_ids == pos, kvn[pl.ds(b, 1), :], tile).astype(jnp.bfloat16)
            spot[...] = tile.reshape(8, ROWS, LANES)
            q = qs[pl.ds(b * 8, 8), :].astype(jnp.bfloat16)
            os_[pl.ds(b * 8, 8), :] = jnp.where(lane8 <= pos, dot_nt(q, tile) * 0.125, -1e30)
        s = os_[...]
        e = jnp.exp(s - jnp.max(s, axis=-1, keepdims=True))
        os_[...] = e / jnp.sum(e, axis=-1, keepdims=True)
        for b in range(B):
            p = os_[pl.ds(b * 8, 8), :].astype(jnp.bfloat16)
            os_[pl.ds(b * 8, 8), :] = dot_nn(p, recv[l, b // 4, :, b % 4].reshape(SEQ, LANES))

    def attn_out(l, ar):
        o0 = os_[pl.ds(0, B, stride=8), :]
        o1 = os_[pl.ds(1, B, stride=8), :]
        o2 = os_[pl.ds(2, B, stride=8), :]
        oa = jnp.where(left, pltpu.roll(o0, HEAD, 1), o1).astype(jnp.bfloat16)
        ob = pltpu.roll(o2, HEAD, 1)[:, 0:HEAD].astype(jnp.bfloat16)
        send_halves(ar, lambda cols: dot_nn(oa, wo[l, pl.ds(0, LANES), cols]) + dot_nn(ob, wo[l, pl.ds(LANES, HEAD), cols]))

    def send_halves(ar, columns):
        for dx in (1, 0):
            xs = (mx + dx) % 2
            part = columns(pl.ds(pl.multiple_of(WIDE * xs, LANES), WIDE))
            for hy in range(2):
                for c in range(2):
                    psend[ar, 4 * hy + 2 * xs + c] = part[ROWS * hy:ROWS * hy + ROWS, COLS * c:COLS * c + COLS].astype(jnp.bfloat16)
            for d in range(N - 1):
                if PEERS[d][1] == dx:
                    rs_copy(ar, d).start()

    def rs_copy(ar, d):
        t = peers[d]
        return pltpu.make_async_remote_copy(
            src_ref=psend.at[ar, t], dst_ref=rsb.at[ar, d],
            send_sem=ar_ss, recv_sem=rs_rs.at[ar],
            device_id=dev(t), device_id_type=pl.DeviceIdType.MESH)

    def ag_copy(ar, d):
        t = peers[d]
        return pltpu.make_async_remote_copy(
            src_ref=hb.at[ar + 1, me], dst_ref=hb.at[ar + 1, me],
            send_sem=ar_ss, recv_sem=ag_rs.at[ar],
            device_id=dev(t), device_id_type=pl.DeviceIdType.MESH)

    def reduce_all(ar, filler=None):
        if filler is not None:
            filler()
        total = psend[ar, me].astype(jnp.float32)
        landed(rsb.at[ar], rs_rs.at[ar])
        for d in range(N - 1):
            total = total + rsb[ar, d].astype(jnp.float32)
        hb[ar + 1, me] = (hb[ar, me].astype(jnp.float32) + total).astype(jnp.bfloat16)
        for d in range(N - 1):
            ag_copy(ar, d).start()

    def gather_wait(ar):
        landed(rsb.at[ar], ag_rs.at[ar])

    out_refs = (outs1, outs2)

    def write_caches(l):
        def chunk(c, _):
            for i in range(8):
                out_refs[l][c * 8 + i] = recv[l, 2 * c + i // 4, :, i % 4].reshape(SEQ, LANES).T
            return 0
        lax.fori_loop(0, CH, chunk, 0)

    def turn(l, lo, hi):
        def quad(j, _):
            rows = weight_rows(j)
            for w in (wg, wu):
                for k in range(6):
                    cols = pl.ds(TILE * k, TILE)
                    w[l, rows, cols] = w[l, rows, cols].T
            return 0
        lax.fori_loop(lo, hi, quad, 0)

    def turn_projection(l):
        for a in range(3):
            for i in range(12):
                spot = wqkv.at[l, pl.ds(LANES * a, LANES), pl.ds(LANES * i, LANES)]
                spot[...] = spot[...].T

    lane_w = lax.broadcasted_iota(jnp.int32, (B, LANES), 1) < HEAD

    def experts(l, ar, pieces=()):
        norm_into(ar, gm, l)

        def up(j):
            rows = weight_rows(j)
            g = u = None
            for k in range(6):
                cols = pl.ds(TILE * k, TILE)
                x = m_s[:, cols]
                dg, du = dot_nn(x, wg[l, rows, cols]), dot_nn(x, wu[l, rows, cols])
                g, u = (dg, du) if g is None else (g + dg, u + du)
            act[j] = g * jax.nn.sigmoid(g) * u

        logits = dot_nt(m_s[...], wr[l])
        for p in pieces:
            a2a_send(1, p)
        up(0)
        up(1)
        chosen = mask_s[l][:, 0:40] > 0.5
        top = jnp.max(jnp.where(chosen, logits, -jnp.inf), axis=-1, keepdims=True)
        e = jnp.where(chosen, jnp.exp(jnp.where(chosen, logits - top, 0.0)), 0.0)
        gate = e / jnp.sum(e, axis=-1, keepdims=True)
        for j in range(QUADS):
            for i in range(2):
                k = 4 * j + 2 * i
                g0 = jnp.broadcast_to(gate[:, k:k + 1], (B, LANES))
                g1 = jnp.broadcast_to(gate[:, k + 1:k + 2], (B, LANES))
                gx[j, :, pl.ds(LANES * i, LANES)] = jnp.where(left, g0, g1)
        for j in range(2, QUADS):
            up(j)
        landed(wd.at[l], s_d.at[l])
        for j in range(QUADS):
            acts[:, pl.ds(TILE * j, TILE)] = (gx[j] * act[j]).astype(jnp.bfloat16)
        send_halves(ar, lambda cols: dot_nn(acts[...], wd[l, :, cols]))

    SC = jax.named_scope
    with SC("p_proj0"):
        project(0, 0)
    with SC("p_prep1"):
        landed(xk, s_in.at[CH])
        for c in range(CH):
            prep(1, c)
        recv[1, :, me] = send[1, :, me]
    with SC("p_turn0"):
        turn_projection(1)
        landed(wg, s_w.at[0])
        turn(0, 0, 10)
    with SC("p_att0"):
        attend(0)
    with SC("p_aout0"):
        attn_out(0, 0)

    def fill_rs0():
        a2a_send(1, 0)
        a2a_send(1, 1)
        write_caches(0)

    with SC("p_rs0"):
        reduce_all(0, fill_rs0)
    with SC("p_ag0"):
        a2a_send(1, 2)
        a2a_send(1, 3)
        landed(wg, s_w.at[1])
        turn(1, 0, 4)
        gather_wait(0)
    for p in range(4, 7):
        a2a_send(1, p)
    with SC("p_moe0"):
        experts(0, 1)
    with SC("p_rs1"):
        reduce_all(1, lambda: turn(1, 4, 6))
    with SC("p_ag1"):
        a2a_send(1, 7)
        turn(1, 6, 8)
        gather_wait(1)
    with SC("p_proj1"):
        project(1, 2)
    with SC("p_att1"):
        attend_all(1)
    with SC("p_aout1"):
        attn_out(1, 2)
    with SC("p_rs2"):
        reduce_all(2, lambda: write_caches(1))
    with SC("p_ag2"):
        turn(1, 8, 10)
        gather_wait(2)
    with SC("p_moe1"):
        experts(1, 3)
    with SC("p_rs3"):
        reduce_all(3)
    with SC("p_ag3"):
        gather_wait(3)
    with SC("p_end"):
        for j in range(N):
            hid_o[pl.ds(ROWS * (j // 4), ROWS), pl.ds(COLS * (j % 4), COLS)] = hb[4, j]
        landed(send.at[:, :, pl.ds(0, N - 1)], a2a_ss)
        landed(rsb, ar_ss)
        landed(rsb, ar_ss)


def tail_kernel(hid, kv1, kv2, hid_o, k1_o, v1_o, k2_o, v2_o, sem):
    copies = [
        (kv1.at[:, pl.ds(0, HEAD)], k1_o), (kv1.at[:, pl.ds(HEAD, HEAD)], v1_o),
        (kv2.at[:, pl.ds(0, HEAD)], k2_o), (kv2.at[:, pl.ds(HEAD, HEAD)], v2_o),
        (hid, hid_o),
    ]
    cps = [pltpu.make_async_copy(src, dst, sem.at[i]) for i, (src, dst) in enumerate(copies)]
    for cp in cps:
        cp.start()
    for cp in cps:
        cp.wait()


def solution(mesh):
    seq_spec = P('dp', 'tp', None, None)
    head_spec = P('dp', None, 'tp', None)
    col_spec = P(None, None, 'tp')
    ff_spec = P(None, None, None, 'tp')
    cos, sin = rope_tables()

    def local_step(hidden, lengths, choice, keys_one, vals_one, keys_two, vals_two, g_attn, w_q, w_k, w_v, w_o, g_mlp, w_router, w_gate, w_up, w_down):
        bf, f32 = jnp.bfloat16, jnp.float32
        any_spec = pl.BlockSpec(memory_space=pl.ANY)
        vmem_spec = pl.BlockSpec(memory_space=pltpu.VMEM)
        dma = pltpu.SemaphoreType.DMA
        vm = pltpu.VMEM
        operands = (
            lengths, hidden, jnp.swapaxes(choice, 1, 2),
            keys_one.reshape(SLOTS, 8, HEAD), vals_one.reshape(SLOTS, 8, HEAD), keys_two.reshape(SLOTS, 8, HEAD), vals_two.reshape(SLOTS, 8, HEAD),
            g_attn, jnp.swapaxes(w_q, 1, 2), jnp.swapaxes(w_k, 1, 2), jnp.swapaxes(w_v, 1, 2), w_o, g_mlp, jnp.swapaxes(w_router, 1, 2),
            jnp.swapaxes(w_gate, 2, 3).reshape(2, 2560, D), jnp.swapaxes(w_up, 2, 3).reshape(2, 2560, D), w_down.reshape(2, 2560, D),
            jnp.asarray(cos), jnp.asarray(sin),
        )
        hid, kv1, kv2 = pl.pallas_call(
            kernel,
            name='decode_two',
            out_shape=[vm((B, D), bf), vm((B, LANES, LANES), bf), vm((B, LANES, LANES), bf)],
            in_specs=[any_spec] * 19,
            out_specs=[vmem_spec] * 3,
            scratch_shapes=[
                pltpu.SMEM((B,), jnp.int32),
                vm((2, 2560, D), bf), vm((2, 2560, D), bf), vm((2, 2560, D), bf),
                vm((2, COLS, D), bf), vm((2, 192, D), bf), vm((2, 40, D), bf),
                vm((2, SLOTS, 8, HEAD), bf), vm((2, SLOTS, 8, HEAD), bf), vm((1024, LANES), f32),
                vm((2, TP, 8, 4, ROWS, LANES), bf), vm((2, TP, 8, 4, ROWS, LANES), bf),
                vm((5, 8, ROWS, COLS), bf), vm((4, 8, ROWS, COLS), bf), vm((4, 7, ROWS, COLS), bf),
                vm((B, D), bf), vm((TILE, LANES), f32), vm((TILE, LANES), f32), vm((B, LANES), f32),
                vm((LANES, LANES), f32), vm((LANES, LANES), f32), vm((B, LANES), f32), vm((B, LANES), f32),
                vm((2, 8, B), jnp.int32), vm((2, D), bf), vm((2, D), bf),
                vm((2, B, LANES), f32), vm((QUADS, B, TILE), f32), vm((QUADS, B, TILE), f32), vm((B, 2560), bf),
                dma((CH + 1,)), dma((2,)), dma((2,)), dma, dma, dma((CH + 1,)), dma, dma((4,)), dma((4,)),
            ],
            compiler_params=pltpu.CompilerParams(collective_id=0, has_side_effects=True, vmem_limit_bytes=63500000),
        )(*operands)
        hid_out, *caches = pl.pallas_call(
            tail_kernel,
            name='write_out',
            out_shape=[jax.ShapeDtypeStruct((B, D), bf)] + [jax.ShapeDtypeStruct((B, HEAD, LANES), bf)] * 4,
            in_specs=[vmem_spec] * 3,
            out_specs=[any_spec] * 5,
            scratch_shapes=[dma((5,))],
            compiler_params=pltpu.CompilerParams(vmem_limit_bytes=4 << 20),
        )(hid, kv1, kv2)
        return (hid_out, *[jnp.swapaxes(kv, 1, 2)[:, :, None, :] for kv in caches])

    return jax.shard_map(local_step, mesh=mesh, in_specs=(P('dp', None), P('dp'), P(None, 'dp', None), seq_spec, seq_spec, seq_spec, seq_spec, P(), col_spec, col_spec, col_spec, P(None, 'tp', None), P(), P(), ff_spec, ff_spec, P(None, None, 'tp', None)), out_specs=(P('dp', None), head_spec, head_spec, head_spec, head_spec), check_vma=False)
```
